32 devices in a mesh: stage: 1 (over z), data: 32 (over y, x, core).
Axes of the slice: x: 4, y: 4, z: 1, core: 2. Of those that a mesh axis runs over, the one named last changes fastest.
The devices are a block of a 4x4x8 slice.
Arguments:
- w_master: float32 [64, 512, 512], P('stage', 'data')
- momentum: float32 [64, 512, 512], P('stage', 'data')
- grads: bfloat16 [32, 64, 512, 512], P(('stage', 'data'))
Outputs:
- output 1: float32 [64, 512, 512], P('stage', 'data')
- output 2: float32 [64, 512, 512], P('stage', 'data')
All inputs are finite; a program needn't handle non-finite values.
Results may differ from the reference program's by a relative error of at most 0.0147319.
Values are sent between devices in bfloat16 or wider.
A program may use at most 768 MiB of HBM per device.

```python
import math
import jax
import jax.numpy as jnp
from jax import lax

GROUP_SIZE = 32
NUM_MATS = 64
MAT_ROWS = 512
MAT_COLS = 512
NS_ITERS = 5

MOMENTUM_COEF = 0.95
LEARN_RATE = 0.05
WEIGHT_DECAY = 0.2
NORM_EPS = 1e-7
COEF_A = 3.4445
COEF_B = -4.7750
COEF_C = 2.0315
RMS_SCALE = 0.2 * math.sqrt(max(MAT_ROWS, MAT_COLS))


def setup_inputs(seed: int = 0, part: int = 0) -> dict:
    base_key = jax.random.fold_in(jax.random.key(seed), part)
    sub_keys = jax.random.split(base_key, 6)
    mat_shape = (NUM_MATS, MAT_ROWS, MAT_COLS)
    w_master = 0.02 * jax.random.normal(sub_keys[0], mat_shape, jnp.float32)
    noise_base = jax.random.normal(sub_keys[1], mat_shape, jnp.float32)
    low_left = jax.random.normal(sub_keys[2], (NUM_MATS, MAT_ROWS, 4), jnp.float32)
    low_right = jax.random.normal(sub_keys[3], (NUM_MATS, 4, MAT_COLS), jnp.float32)
    shared = 0.25 * jnp.einsum('mrk,mkc->mrc', low_left, low_right)
    row_scale = jax.random.uniform(sub_keys[4], (NUM_MATS, MAT_ROWS, 1), jnp.float32, 0.5, 1.5)
    momentum = row_scale * (noise_base + shared)
    grads = (jax.random.normal(sub_keys[5], (GROUP_SIZE,) + mat_shape, jnp.float32) * GROUP_SIZE ** -0.5).astype(jnp.bfloat16)
    return {'w_master': w_master, 'momentum': momentum, 'grads': grads}


def newton_schulz(x_start):
    is_tall = MAT_ROWS > MAT_COLS
    x_cur = x_start.T if is_tall else x_start
    for _ in range(NS_ITERS):
        gram_mat = jnp.dot(x_cur, x_cur.T, preferred_element_type=jnp.float32).astype(jnp.bfloat16)
        gram_sq = jnp.dot(gram_mat, gram_mat, preferred_element_type=jnp.float32)
        poly_mat = (COEF_B * gram_mat.astype(jnp.float32) + COEF_C * gram_sq).astype(jnp.bfloat16)
        poly_x = jnp.dot(poly_mat, x_cur, preferred_element_type=jnp.float32)
        x_cur = (COEF_A * x_cur.astype(jnp.float32) + poly_x).astype(jnp.bfloat16)
    return x_cur.T if is_tall else x_cur


def reference(w_master, momentum, grads):
    grad_sum = jnp.sum(grads.astype(jnp.float32), axis=0)
    mom_new = MOMENTUM_COEF * momentum + grad_sum
    frob_norm = jnp.sqrt(jnp.sum(mom_new * mom_new, axis=(1, 2)))

    def one_matrix(mat_pair):
        mom_one, norm_one = mat_pair
        x_start = (mom_one.astype(jnp.bfloat16).astype(jnp.float32) / (norm_one + NORM_EPS)).astype(jnp.bfloat16)
        return newton_schulz(x_start)

    x_ortho = lax.map(one_matrix, (mom_new, frob_norm))
    w_new = w_master - LEARN_RATE * (x_ortho.astype(jnp.float32) * RMS_SCALE + WEIGHT_DECAY * w_master)
    return w_new, mom_new
```

```python
import functools
import math

import jax
import jax.numpy as jnp
from jax import lax
from jax.experimental import pallas as pl
from jax.experimental.pallas import tpu as pltpu
from jax.sharding import PartitionSpec as P

MOMENTUM_COEF = 0.95
LEARN_RATE = 0.05
WEIGHT_DECAY = 0.2
NORM_EPS = 1e-7
COEF_A = 3.4445
COEF_B = -4.7750
COEF_C = 2.0315
NS_ITERS = 5

CORES = 2
RING = 4
SIGNS = (1, -1, 1, -1)
X_FIRST = (True, True, False, False)
GROUPS = 4
PER_GROUP = 1
IN_SLOTS = 6
SEND_SLOTS = 3
AHEAD = 2
MESH = pl.DeviceIdType.MESH


def _kernel(
    devs, grads, mom_in, mom_out, rows_out,
    own, peer, r1, r2, r3, p1, p2, p3, lead, mom, half_out, sq_out, half_in, sq_in, x_buf, gram, poly,
    own_sem, peer_send, peer_recv, peer_free, lead_send, r_recv, fwd_send, p_recv, part_send, last_send,
    mom_sem, mom_done, half_send, sq_send, half_recv, sq_recv, x_send, x_recv, x_self,
):
    n_mats, rows, cols = mom.shape
    q = PER_GROUP
    m = GROUPS * q
    chunks = n_mats // m
    slots = n_mats // devs
    f32, bf16 = jnp.float32, jnp.bfloat16

    me = lax.axis_index('data')
    core = lax.rem(me, CORES)
    chip = me // CORES
    px, py = lax.rem(chip, RING), chip // RING
    buddy = me + 1 - 2 * core

    def at(pos, step):
        return lax.rem(pos + step + RING, RING)

    def device(x, y):
        return (y * RING + x) * CORES + core

    def first(g):
        return px if X_FIRST[g] else py

    def second(g):
        return py if X_FIRST[g] else px

    def chip_of(g, on_first, on_second):
        x, y = (on_first, on_second) if X_FIRST[g] else (on_second, on_first)
        return y * RING + x

    def near_first(g, step):
        return device(at(px, step), py) if X_FIRST[g] else device(px, at(py, step))

    def near_second(g, step):
        return device(px, at(py, step)) if X_FIRST[g] else device(at(px, step), py)

    def remote(src, dst, send, recv, target):
        return pltpu.make_async_remote_copy(
            src_ref=src, dst_ref=dst, send_sem=send, recv_sem=recv,
            device_id={'data': target}, device_id_type=MESH)

    def wait_bytes(ref, sem):
        pltpu.make_async_copy(ref, ref, sem).wait()

    def owner_of(j):
        jj = lax.rem(j, devs)
        return lax.rem(jj, RING) * (devs // RING) + jj // RING

    barrier = pltpu.get_barrier_semaphore()

    @pl.loop(1, devs)
    def _(i):
        pl.semaphore_signal(barrier, inc=1, device_id={'data': lax.rem(me + i, devs)}, device_id_type=MESH)

    pl.semaphore_wait(barrier, devs - 1)

    def fetch(k):
        slot = lax.rem(k, IN_SLOTS)
        pltpu.make_async_copy(grads.at[pl.ds(k * m, m), :, core], own.at[slot], own_sem.at[slot]).start()

        @pl.when(k >= IN_SLOTS)
        def _():
            pl.semaphore_wait(peer_free, 1)

        remote(grads.at[pl.ds(k * m, m), :, 1 - core], peer.at[slot], peer_send.at[slot], peer_recv.at[slot], buddy).start()

    def pair(slot, g, i, on_first, o):
        c = chip_of(g, on_first, o)
        return own[slot, g * q + i, c].astype(f32) + peer[slot, g * q + i, c].astype(f32)

    def lead_stage(k):
        slot, st = lax.rem(k, IN_SLOTS), lax.rem(k, SEND_SLOTS)
        wait_bytes(own.at[slot], own_sem.at[slot])
        wait_bytes(peer.at[slot], peer_send.at[slot])
        wait_bytes(peer.at[slot], peer_recv.at[slot])

        @pl.when(k >= SEND_SLOTS)
        def _():
            wait_bytes(lead.at[st], lead_send.at[st])

        for role, step in ((0, 2), (1, -1)):
            for g in range(GROUPS):
                dest = at(first(g), step * SIGNS[g])
                for o in range(RING):
                    for i in range(q):
                        lead[st, role, g, o, i] = pair(slot, g, i, dest, o)
        for g in range(GROUPS):
            remote(lead.at[st, 0, g], r1.at[k, g], lead_send.at[st], r_recv.at[0, k], near_first(g, SIGNS[g])).start()
            remote(lead.at[st, 1, g], r2.at[k, g], lead_send.at[st], r_recv.at[1, k], near_first(g, -SIGNS[g])).start()

    def forward_stage(k):
        slot = lax.rem(k, IN_SLOTS)
        wait_bytes(r1.at[k], r_recv.at[0, k])
        for g in range(GROUPS):
            dest = at(first(g), SIGNS[g])
            for o in range(RING):
                for i in range(q):
                    r1[k, g, o, i] = r1[k, g, o, i] + pair(slot, g, i, dest, o)
        for g in range(GROUPS):
            remote(r1.at[k, g], r3.at[k, g], fwd_send.at[k], r_recv.at[2, k], near_first(g, SIGNS[g])).start()

    def part_stage(k):
        slot = lax.rem(k, IN_SLOTS)
        wait_bytes(r2.at[k], r_recv.at[1, k])
        wait_bytes(r3.at[k], r_recv.at[2, k])
        for g in range(GROUPS):
            for o in range(RING):
                for i in range(q):
                    r3[k, g, o, i] = (r3[k, g, o, i] + r2[k, g, o, i]) + pair(slot, g, i, first(g), o)

        @pl.when(k + IN_SLOTS < chunks)
        def _():
            pl.semaphore_signal(peer_free, inc=1, device_id={'data': buddy}, device_id_type=MESH)

        for g in range(GROUPS):
            s = SIGNS[g]
            remote(r3.at[k, g, at(second(g), 2 * s)], p1.at[k, g], part_send.at[k], p_recv.at[0, k], near_second(g, s)).start()
            remote(r3.at[k, g, at(second(g), -s)], p2.at[k, g], part_send.at[k], p_recv.at[1, k], near_second(g, -s)).start()

    def last_stage(k):
        wait_bytes(p1.at[k], p_recv.at[0, k])
        for g in range(GROUPS):
            dest = at(second(g), SIGNS[g])
            for i in range(q):
                p1[k, g, i] = p1[k, g, i] + r3[k, g, dest, i]
        for g in range(GROUPS):
            remote(p1.at[k, g], p3.at[k, g], last_send.at[k], p_recv.at[2, k], near_second(g, SIGNS[g])).start()

    def final_stage(k):
        @pl.when(k == 0)
        def _():
            wait_bytes(mom, mom_sem)

        wait_bytes(p2.at[k], p_recv.at[1, k])
        wait_bytes(p3.at[k], p_recv.at[2, k])
        for g in range(GROUPS):
            for i in range(q):
                j = k * m + g * q + i
                total = r3[k, g, second(g), i] + p2[k, g, i] + p3[k, g, i]
                new = MOMENTUM_COEF * mom[j] + total
                mom[j] = new
                short = new.astype(bf16)
                sq = jnp.sum(new * new, axis=0, keepdims=True)
                sq = functools.reduce(jnp.add, [sq[:, n * 128:(n + 1) * 128] for n in range(cols // 128)])
                half_out[j] = short
                sq_out[j] = sq
                owner, slot = owner_of(j), j // devs

                @pl.when(owner == me)
                def _():
                    half_in[slot, me] = short
                    sq_in[slot, me] = sq

        pltpu.make_async_copy(mom.at[pl.ds(k * m, m)], mom_out.at[pl.ds(k * m, m)], mom_done).start()

        for n in range(m):
            j = k * m + n
            owner, slot = owner_of(j), j // devs

            @pl.when(owner != me)
            def _():
                remote(half_out.at[j], half_in.at[slot, me], half_send, half_recv.at[slot], owner).start()
                remote(sq_out.at[j], sq_in.at[slot, me], sq_send, sq_recv.at[slot], owner).start()

    def ns_start(slot):
        wait_bytes(half_in.at[slot, pl.ds(0, devs - 1)], half_recv.at[slot])
        wait_bytes(sq_in.at[slot, pl.ds(0, devs - 1)], sq_recv.at[slot])
        sq = jnp.sum(jnp.sum(sq_in[slot], axis=0), axis=1, keepdims=True)
        scale = jnp.sqrt(sq) + NORM_EPS

        @pl.loop(0, devs)
        def _(d):
            x_buf[slot, pl.ds(pl.multiple_of(d * rows, rows), rows), :] = (half_in[slot, d].astype(f32) / scale).astype(bf16)

    def ns_iter(slot):
        x = x_buf[slot]
        gram[...] = lax.dot_general(x, x, (((1,), (1,)), ((), ())), preferred_element_type=f32).astype(bf16)
        a = gram[...]
        poly[...] = (COEF_B * a.astype(f32) + COEF_C * jnp.dot(a, a, preferred_element_type=f32)).astype(bf16)
        x_buf[slot] = (COEF_A * x.astype(f32) + jnp.dot(poly[...], x, preferred_element_type=f32)).astype(bf16)

    def mat_of(slot, d):
        return slot * devs + lax.rem(d, devs // RING) * RING + d // (devs // RING)

    def x_block(slot, d):
        return x_buf.at[slot, pl.ds(pl.multiple_of(d * rows, rows), rows), :]

    def x_give(slot):
        j = mat_of(slot, me)

        @pl.loop(1, devs)
        def _(i):
            d = lax.rem(me + i, devs)
            remote(x_block(slot, d), rows_out.at[j], x_send.at[slot], x_recv.at[slot], d).start()

        pltpu.make_async_copy(x_block(slot, me), rows_out.at[j], x_self.at[slot]).start()

    pltpu.make_async_copy(mom_in, mom, mom_sem).start()
    for k in range(AHEAD):
        fetch(jnp.int32(k))

    ns_at = chunks // slots + 4
    steps = max(chunks + 4, ns_at + NS_ITERS)

    @pl.loop(0, steps)
    def _(t):
        @pl.when(t + AHEAD < chunks)
        def _():
            fetch(t + AHEAD)

        for lag, stage in enumerate((lead_stage, forward_stage, part_stage, last_stage, final_stage)):
            @pl.when(jnp.logical_and(t >= lag, t < chunks + lag))
            def _():
                stage(t - lag)

        @pl.when(t == ns_at)
        def _():
            ns_start(0)

        @pl.when(jnp.logical_and(t >= ns_at, t < ns_at + NS_ITERS))
        def _():
            ns_iter(0)

        @pl.when(t == ns_at + NS_ITERS - 1)
        def _():
            x_give(0)

    for slot in range(1, slots):
        ns_start(slot)

        @pl.loop(0, NS_ITERS)
        def _(i):
            ns_iter(slot)

        x_give(slot)

    @pl.loop(0, chunks)
    def _(k):
        wait_bytes(r1.at[k], fwd_send.at[k])
        wait_bytes(p1.at[k], part_send.at[k])
        wait_bytes(p2.at[k], part_send.at[k])
        wait_bytes(p1.at[k], last_send.at[k])

    for st in range(SEND_SLOTS):
        wait_bytes(lead.at[st], lead_send.at[st])
    wait_bytes(mom, mom_done)
    wait_bytes(half_out.at[pl.ds(0, n_mats - slots)], half_send)
    wait_bytes(sq_out.at[pl.ds(0, n_mats - slots)], sq_send)
    for slot in range(slots):
        wait_bytes(half_in.at[slot, pl.ds(0, devs - 1)], x_send.at[slot])
        wait_bytes(half_in.at[slot, pl.ds(0, devs - 1)], x_recv.at[slot])
        pltpu.make_async_copy(x_block(slot, 0), rows_out.at[0], x_self.at[slot]).wait()


def exchange(devs, grads, mom):
    n_mats, rows, cols = mom.shape
    n_rows = rows * devs
    chips = devs // CORES
    q = PER_GROUP
    m = GROUPS * q
    chunks = n_mats // m
    slots = n_mats // devs
    f32, bf16 = jnp.float32, jnp.bfloat16
    dma, vmem = pltpu.SemaphoreType.DMA, pltpu.VMEM
    grads = grads.reshape(n_mats, chips, CORES, rows, cols)
    wide = (chunks, GROUPS, RING, q, rows, cols)
    thin = (chunks, GROUPS, q, rows, cols)
    return pl.pallas_call(
        functools.partial(_kernel, devs),
        out_shape=(
            jax.ShapeDtypeStruct(mom.shape, f32),
            jax.ShapeDtypeStruct(mom.shape, bf16),
        ),
        in_specs=[pl.BlockSpec(memory_space=pl.ANY)] * 2,
        out_specs=(pl.BlockSpec(memory_space=pl.ANY),) * 2,
        scratch_shapes=[
            vmem((IN_SLOTS, m, chips, rows, cols), bf16),
            vmem((IN_SLOTS, m, chips, rows, cols), bf16),
            vmem(wide, f32), vmem(wide, f32), vmem(wide, f32),
            vmem(thin, f32), vmem(thin, f32), vmem(thin, f32),
            vmem((SEND_SLOTS, 2, GROUPS, RING, q, rows, cols), f32),
            vmem(mom.shape, f32),
            vmem(mom.shape, bf16),
            vmem((n_mats, 1, 128), f32),
            vmem((slots, devs, rows, cols), bf16),
            vmem((slots, devs, 1, 128), f32),
            vmem((slots, n_rows, cols), bf16),
            vmem((n_rows, n_rows), bf16),
            vmem((n_rows, n_rows), bf16),
            dma((IN_SLOTS,)), dma((IN_SLOTS,)), dma((IN_SLOTS,)), pltpu.SemaphoreType.REGULAR,
            dma((SEND_SLOTS,)), dma((3, chunks)), dma((chunks,)), dma((3, chunks)), dma((chunks,)), dma((chunks,)),
            dma, dma, dma, dma, dma((slots,)), dma((slots,)), dma((slots,)), dma((slots,)), dma((slots,)),
        ],
        compiler_params=pltpu.CompilerParams(
            collective_id=0, has_side_effects=True, vmem_limit_bytes=67043328),
    )(grads, mom)


def solution(mesh):
    devs = mesh.shape['data']
    row_spec = P('stage', 'data', None)
    grad_spec = P(('stage', 'data'), None, None, None)

    def local_step(w_rows, mom_rows, grad_full):
        n_mats, rows_dev, n_cols = w_rows.shape
        n_rows = rows_dev * devs
        assert devs == RING * RING * CORES and n_rows <= n_cols
        mom_new, x_rows = exchange(devs, grad_full[0], mom_rows)
        rms_scale = 0.2 * math.sqrt(max(n_rows, n_cols))
        w_new = w_rows - LEARN_RATE * (x_rows.astype(jnp.float32) * rms_scale + WEIGHT_DECAY * w_rows)
        return w_new, mom_new

    return jax.shard_map(local_step, mesh=mesh, in_specs=(row_spec, row_spec, grad_spec), out_specs=(row_spec, row_spec), check_vma=False)
```

```python
import functools
import math

import jax
import jax.numpy as jnp
from jax import lax
from jax.experimental import pallas as pl
from jax.experimental.pallas import tpu as pltpu
from jax.sharding import PartitionSpec as P

MOMENTUM_COEF = 0.95
LEARN_RATE = 0.05
WEIGHT_DECAY = 0.2
NORM_EPS = 1e-7
COEF_A = 3.4445
COEF_B = -4.7750
COEF_C = 2.0315
NS_ITERS = 5

CORES = 2
RING = 4
SIGNS = (1, -1, 1, -1)
X_FIRST = (True, True, False, False)
GROUPS = 4
IN_SLOTS = 6
SEND_SLOTS = 3
AHEAD = 2
MESH = pl.DeviceIdType.MESH


def _kernel(
    devs, grads, mom_in, w_in, mom_out, w_out,
    own, peer, r1, r2, r3, p1, p2, p3, lead, mom, w, half_out, sq_out, half_in, sq_in, x_buf, x_in, gram, poly,
    own_sem, peer_send, peer_recv, peer_free, lead_send, r_recv, fwd_send, p_recv, part_send, last_send,
    mom_sem, mom_done, w_sem, w_done, half_send, sq_send, half_recv, sq_recv, x_send, x_recv0, x_recv,
):
    n_mats, rows, cols = mom.shape
    m = GROUPS
    chunks = n_mats // m
    slots = n_mats // devs
    per_slot = chunks // slots
    rms_scale = 0.2 * math.sqrt(max(rows * devs, cols))
    f32, bf16 = jnp.float32, jnp.bfloat16

    me = lax.axis_index('data')
    core = lax.rem(me, CORES)
    chip = me // CORES
    px, py = lax.rem(chip, RING), chip // RING
    buddy = me + 1 - 2 * core

    def at(pos, step):
        return lax.rem(pos + step + RING, RING)

    def device(x, y):
        return (y * RING + x) * CORES + core

    def first(g):
        return px if X_FIRST[g] else py

    def second(g):
        return py if X_FIRST[g] else px

    def chip_of(g, on_first, on_second):
        x, y = (on_first, on_second) if X_FIRST[g] else (on_second, on_first)
        return y * RING + x

    def near_first(g, step):
        return device(at(px, step), py) if X_FIRST[g] else device(px, at(py, step))

    def near_second(g, step):
        return device(px, at(py, step)) if X_FIRST[g] else device(at(px, step), py)

    def remote(src, dst, send, recv, target):
        return pltpu.make_async_remote_copy(
            src_ref=src, dst_ref=dst, send_sem=send, recv_sem=recv,
            device_id={'data': target}, device_id_type=MESH)

    def wait_bytes(ref, sem):
        pltpu.make_async_copy(ref, ref, sem).wait()

    def owner_of(k, g):
        kk = lax.rem(k, per_slot)
        return (g * RING + lax.rem(kk + g, RING)) * CORES + kk // RING

    my_turn = RING * core + at(px, -py)

    def mine(slot):
        return (slot * per_slot + my_turn) * m + py

    def fetch_own(k):
        slot = lax.rem(k, IN_SLOTS)
        pltpu.make_async_copy(grads.at[pl.ds(k * m, m), :, core], own.at[slot], own_sem.at[slot]).start()

    def fetch_peer(k):
        slot = lax.rem(k, IN_SLOTS)

        @pl.when(k >= IN_SLOTS)
        def _():
            pl.semaphore_wait(peer_free, 1)

        remote(grads.at[pl.ds(k * m, m), :, 1 - core], peer.at[slot], peer_send.at[slot], peer_recv.at[slot], buddy).start()

    def pair(slot, g, on_first, o):
        c = chip_of(g, on_first, o)
        return own[slot, g, c].astype(f32) + peer[slot, g, c].astype(f32)

    def lead_stage(k):
        slot, st = lax.rem(k, IN_SLOTS), lax.rem(k, SEND_SLOTS)
        wait_bytes(own.at[slot], own_sem.at[slot])
        wait_bytes(peer.at[slot], peer_send.at[slot])
        wait_bytes(peer.at[slot], peer_recv.at[slot])

        @pl.when(k >= SEND_SLOTS)
        def _():
            wait_bytes(lead.at[st], lead_send.at[st])

        for role, step in ((0, 2), (1, -1)):
            for g in range(GROUPS):
                dest = at(first(g), step * SIGNS[g])
                for o in range(RING):
                    lead[st, role, g, o] = pair(slot, g, dest, o)
            for g in range(GROUPS):
                into, toward = ((r1, SIGNS[g]), (r2, -SIGNS[g]))[role]
                remote(lead.at[st, role, g], into.at[k, g], lead_send.at[st], r_recv.at[role, k], near_first(g, toward)).start()

    def forward_stage(k):
        slot = lax.rem(k, IN_SLOTS)
        wait_bytes(r1.at[k], r_recv.at[0, k])
        for g in range(GROUPS):
            dest = at(first(g), SIGNS[g])
            for o in range(RING):
                r1[k, g, o] = r1[k, g, o] + pair(slot, g, dest, o)
        for g in range(GROUPS):
            remote(r1.at[k, g], r3.at[k, g], fwd_send.at[k], r_recv.at[2, k], near_first(g, SIGNS[g])).start()

    def part_stage(k):
        slot = lax.rem(k, IN_SLOTS)
        wait_bytes(r2.at[k], r_recv.at[1, k])
        wait_bytes(r3.at[k], r_recv.at[2, k])
        for g in range(GROUPS):
            for o in range(RING):
                r3[k, g, o] = (r3[k, g, o] + r2[k, g, o]) + pair(slot, g, first(g), o)

        @pl.when(k + IN_SLOTS < chunks)
        def _():
            pl.semaphore_signal(peer_free, inc=1, device_id={'data': buddy}, device_id_type=MESH)

        for g in range(GROUPS):
            s = SIGNS[g]
            remote(r3.at[k, g, at(second(g), 2 * s)], p1.at[k, g], part_send.at[k], p_recv.at[0, k], near_second(g, s)).start()
            remote(r3.at[k, g, at(second(g), -s)], p2.at[k, g], part_send.at[k], p_recv.at[1, k], near_second(g, -s)).start()

    def last_stage(k):
        wait_bytes(p1.at[k], p_recv.at[0, k])
        for g in range(GROUPS):
            dest = at(second(g), SIGNS[g])
            p1[k, g] = p1[k, g] + r3[k, g, dest]
        for g in range(GROUPS):
            remote(p1.at[k, g], p3.at[k, g], last_send.at[k], p_recv.at[2, k], near_second(g, SIGNS[g])).start()

    def final_stage(k):
        @pl.when(k == 0)
        def _():
            wait_bytes(mom, mom_sem)

        wait_bytes(p2.at[k], p_recv.at[1, k])
        wait_bytes(p3.at[k], p_recv.at[2, k])
        for g in range(GROUPS):
            j = k * m + g
            total = r3[k, g, second(g)] + p2[k, g] + p3[k, g]
            new = MOMENTUM_COEF * mom[j] + total
            mom[j] = new
            short = new.astype(bf16)
            sq = jnp.sum(new * new, axis=0, keepdims=True)
            sq = functools.reduce(jnp.add, [sq[:, n * 128:(n + 1) * 128] for n in range(cols // 128)])
            half_out[j] = short
            sq_out[j] = sq

            @pl.when(owner_of(k, g) == me)
            def _():
                half_in[k // per_slot, me] = short
                sq_in[k // per_slot, me] = sq

        for g in range(GROUPS):
            j, slot, owner = k * m + g, k // per_slot, owner_of(k, g)

            @pl.when(owner != me)
            def _():
                remote(half_out.at[j], half_in.at[slot, me], half_send, half_recv.at[slot], owner).start()
                remote(sq_out.at[j], sq_in.at[slot, me], sq_send, sq_recv.at[slot], owner).start()

        pltpu.make_async_copy(mom.at[pl.ds(k * m, m)], mom_out.at[pl.ds(k * m, m)], mom_done).start()

    def ns_start(slot):
        wait_bytes(half_in.at[slot, pl.ds(0, devs - 1)], half_recv.at[slot])
        wait_bytes(sq_in.at[slot, pl.ds(0, devs - 1)], sq_recv.at[slot])
        sq = jnp.sum(jnp.sum(sq_in[slot], axis=0), axis=1, keepdims=True)
        scale = jnp.sqrt(sq) + NORM_EPS

        @pl.loop(0, devs)
        def _(d):
            x_buf[slot, pl.ds(pl.multiple_of(d * rows, rows), rows), :] = (half_in[slot, d].astype(f32) / scale).astype(bf16)

    def ns_iter(slot):
        x = x_buf[slot]
        gram[...] = lax.dot_general(x, x, (((1,), (1,)), ((), ())), preferred_element_type=f32).astype(bf16)
        a = gram[...]
        poly[...] = (COEF_B * a.astype(f32) + COEF_C * jnp.dot(a, a, preferred_element_type=f32)).astype(bf16)
        x_buf[slot] = (COEF_A * x.astype(f32) + jnp.dot(poly[...], x, preferred_element_type=f32)).astype(bf16)

    def x_block(slot, d):
        return x_buf.at[slot, pl.ds(pl.multiple_of(d * rows, rows), rows), :]

    def x_give(slot, part):
        j = mine(slot)
        recv = x_recv0 if slot == 0 else x_recv.at[slot - 1, my_turn]
        for dx in range(RING):
            for c in range(CORES):
                d = (lax.rem(py + dx + part, RING) * RING + lax.rem(px + dx, RING)) * CORES + c

                @pl.when(d != me)
                def _():
                    remote(x_block(slot, d), x_in.at[j], x_send.at[slot], recv, d).start()

    def x_keep(slot):
        x_in[mine(slot)] = x_buf[slot, pl.ds(pl.multiple_of(me * rows, rows), rows), :]

    def update(k):
        for g in range(GROUPS):
            j = k * m + g
            old = w[j]
            w[j] = old - LEARN_RATE * (x_in[j].astype(f32) * rms_scale + WEIGHT_DECAY * old)
        pltpu.make_async_copy(w.at[pl.ds(k * m, m)], w_out.at[pl.ds(k * m, m)], w_done).start()

    for k in range(AHEAD):
        fetch_own(jnp.int32(k))
    barrier = pltpu.get_barrier_semaphore()
    near = (buddy, device(at(px, 1), py), device(at(px, -1), py), device(px, at(py, 1)), device(px, at(py, -1)))
    for d in near:
        pl.semaphore_signal(barrier, inc=1, device_id={'data': d}, device_id_type=MESH)
    pl.semaphore_wait(barrier, len(near))
    for k in range(AHEAD):
        fetch_peer(jnp.int32(k))
    pltpu.make_async_copy(mom_in, mom, mom_sem).start()
    pltpu.make_async_copy(w_in, w, w_sem).start()

    drain = chunks
    ended = chunks + 4

    @pl.loop(0, ended + NS_ITERS)
    def _(t):
        @pl.when(t + AHEAD < chunks)
        def _():
            fetch_own(t + AHEAD)
            fetch_peer(t + AHEAD)

        for lag, stage in enumerate((lead_stage, forward_stage, part_stage, last_stage, final_stage)):
            @pl.when(jnp.logical_and(t >= lag, t < chunks + lag))
            def _():
                stage(t - lag)

        for slot in range(slots):
            begin = slot * per_slot + my_turn + 5

            @pl.when(t == begin)
            def _():
                ns_start(slot)

            @pl.when(jnp.logical_and(t >= begin, t < begin + NS_ITERS))
            def _():
                ns_iter(slot)

            @pl.when(t == begin + NS_ITERS - 1)
            def _():
                x_keep(slot)

            if slot < slots - 1:
                @pl.when(jnp.logical_and(t >= drain, t < drain + RING))
                def _():
                    x_give(slot, t - drain)
            else:
                @pl.when(t == jnp.maximum(begin + NS_ITERS - 1, ended))
                def _():
                    @pl.loop(0, RING)
                    def _(part):
                        x_give(slot, part)

    wait_bytes(w, w_sem)
    wait_bytes(half_in.at[0, pl.ds(0, devs - 1)], x_recv0)

    @pl.loop(0, per_slot)
    def _(k):
        update(k)

    @pl.loop(0, per_slot)
    def _(turn):
        @pl.when(turn == my_turn)
        def _():
            wait_bytes(x_in.at[pl.ds(0, m - 1)], x_recv.at[0, turn])

        @pl.when(turn != my_turn)
        def _():
            wait_bytes(x_in.at[pl.ds(0, m)], x_recv.at[0, turn])

        update(per_slot + turn)

    @pl.loop(0, chunks)
    def _(k):
        wait_bytes(r1.at[k], fwd_send.at[k])
        wait_bytes(p1.at[k], part_send.at[k])
        wait_bytes(p2.at[k], part_send.at[k])
        wait_bytes(p1.at[k], last_send.at[k])

    for st in range(SEND_SLOTS):
        wait_bytes(lead.at[st], lead_send.at[st])
    wait_bytes(half_out.at[pl.ds(0, n_mats - slots)], half_send)
    wait_bytes(sq_out.at[pl.ds(0, n_mats - slots)], sq_send)
    for slot in range(slots):
        wait_bytes(half_in.at[slot, pl.ds(0, devs - 1)], x_send.at[slot])
    wait_bytes(mom, mom_done)
    wait_bytes(w, w_done)


def muon(devs, grads, mom, w):
    n_mats, rows, cols = mom.shape
    n_rows = rows * devs
    chips = devs // CORES
    m = GROUPS
    chunks = n_mats // m
    slots = n_mats // devs
    f32, bf16 = jnp.float32, jnp.bfloat16
    dma, vmem = pltpu.SemaphoreType.DMA, pltpu.VMEM
    grads = grads.reshape(n_mats, chips, CORES, rows, cols)
    wide = (chunks, GROUPS, RING, rows, cols)
    thin = (chunks, GROUPS, rows, cols)
    return pl.pallas_call(
        functools.partial(_kernel, devs),
        out_shape=(
            jax.ShapeDtypeStruct(mom.shape, f32),
            jax.ShapeDtypeStruct(w.shape, f32),
        ),
        in_specs=[pl.BlockSpec(memory_space=pl.ANY)] * 3,
        out_specs=(pl.BlockSpec(memory_space=pl.ANY),) * 2,
        scratch_shapes=[
            vmem((IN_SLOTS, m, chips, rows, cols), bf16),
            vmem((IN_SLOTS, m, chips, rows, cols), bf16),
            vmem(wide, f32), vmem(wide, f32), vmem(wide, f32),
            vmem(thin, f32), vmem(thin, f32), vmem(thin, f32),
            vmem((SEND_SLOTS, 2, GROUPS, RING, rows, cols), f32),
            vmem(mom.shape, f32),
            vmem(w.shape, f32),
            vmem(mom.shape, bf16),
            vmem((n_mats, 1, 128), f32),
            vmem((slots, devs, rows, cols), bf16),
            vmem((slots, devs, 1, 128), f32),
            vmem((slots, n_rows, cols), bf16),
            vmem(mom.shape, bf16),
            vmem((n_rows, n_rows), bf16),
            vmem((n_rows, n_rows), bf16),
            dma((IN_SLOTS,)), dma((IN_SLOTS,)), dma((IN_SLOTS,)), pltpu.SemaphoreType.REGULAR,
            dma((SEND_SLOTS,)), dma((3, chunks)), dma((chunks,)), dma((3, chunks)), dma((chunks,)), dma((chunks,)),
            dma, dma, dma, dma, dma, dma, dma((slots,)), dma((slots,)), dma((slots,)), dma, dma((slots - 1, chunks // slots)),
        ],
        compiler_params=pltpu.CompilerParams(
            collective_id=0, has_side_effects=True, vmem_limit_bytes=67043328),
    )(grads, mom, w)


def solution(mesh):
    devs = mesh.shape['data']
    row_spec = P('stage', 'data', None)
    grad_spec = P(('stage', 'data'), None, None, None)

    def local_step(w_rows, mom_rows, grad_full):
        n_mats, rows_dev, n_cols = w_rows.shape
        assert devs == RING * RING * CORES and n_mats == 2 * devs and rows_dev * devs <= n_cols
        mom_new, w_new = muon(devs, grad_full[0], mom_rows, w_rows)
        return w_new, mom_new

    return jax.shard_map(local_step, mesh=mesh, in_specs=(row_spec, row_spec, grad_spec), out_specs=(row_spec, row_spec), check_vma=False)
```

```python
import functools
import math

import jax
import jax.numpy as jnp
from jax import lax
from jax.experimental import pallas as pl
from jax.experimental.pallas import tpu as pltpu
from jax.sharding import PartitionSpec as P

MOMENTUM_COEF = 0.95
LEARN_RATE = 0.05
WEIGHT_DECAY = 0.2
NORM_EPS = 1e-7
COEF_A = 3.4445
COEF_B = -4.7750
COEF_C = 2.0315
NS_ITERS = 5
EARLY = 3

CORES = 2
RING = 4
SIGNS = (1, -1, 1, -1)
X_FIRST = (True, True, False, False)
GROUPS = 4
IN_SLOTS = 6
SEND_SLOTS = 3
AHEAD = 2
MESH = pl.DeviceIdType.MESH


def _kernel(
    devs, grads, mom_in, w_in, mom, w,
    own, peer, r1, r2, r3, p1, p2, p3, lead, raw, half_out, sq_out, half_in, sq_in, x_buf, x_in, gram, poly,
    own_sem, peer_send, peer_recv, peer_free, lead_send, raw_send, r_recv, fwd_send, p_recv, part_send, last_send,
    mom_sem, w_sem, half_send, sq_send, half_recv, sq_recv, x_send, x_recv0, x_recv,
):
    n_mats, rows, cols = mom.shape
    m = GROUPS
    chunks = n_mats // m
    slots = n_mats // devs
    per_slot = chunks // slots
    rms_scale = 0.2 * math.sqrt(max(rows * devs, cols))
    f32, bf16 = jnp.float32, jnp.bfloat16

    me = lax.axis_index('data')
    core = lax.rem(me, CORES)
    chip = me // CORES
    px, py = lax.rem(chip, RING), chip // RING
    buddy = me + 1 - 2 * core

    def at(pos, step):
        return lax.rem(pos + step + RING, RING)

    def device(x, y):
        return (y * RING + x) * CORES + core

    def first(g):
        return px if X_FIRST[g] else py

    def second(g):
        return py if X_FIRST[g] else px

    def near_first(g, step):
        return device(at(px, step), py) if X_FIRST[g] else device(px, at(py, step))

    def near_second(g, step):
        return device(px, at(py, step)) if X_FIRST[g] else device(at(px, step), py)

    def remote(src, dst, send, recv, target):
        return pltpu.make_async_remote_copy(
            src_ref=src, dst_ref=dst, send_sem=send, recv_sem=recv,
            device_id={'data': target}, device_id_type=MESH)

    def wait_bytes(ref, sem):
        pltpu.make_async_copy(ref, ref, sem).wait()

    def owner_of(k, g):
        kk = lax.rem(k, per_slot)
        return (g * RING + lax.rem(kk + g, RING)) * CORES + kk // RING

    my_turn = RING * core + at(px, -py)

    def mine(slot):
        return (slot * per_slot + my_turn) * m + py

    def fetch_own(k):
        slot = lax.rem(k, IN_SLOTS)
        pltpu.make_async_copy(grads.at[pl.ds(k * m, m), :, :, core], own.at[slot], own_sem.at[slot]).start()

    def fetch_peer(k):
        slot = lax.rem(k, IN_SLOTS)

        @pl.when(k >= IN_SLOTS)
        def _():
            pl.semaphore_wait(peer_free, 1)

        remote(grads.at[pl.ds(k * m, m), :, :, 1 - core], peer.at[slot], peer_send.at[slot], peer_recv.at[slot], buddy).start()

    def pair(slot, g, on_first, o):
        y, x = (o, on_first) if X_FIRST[g] else (on_first, o)
        return own[slot, g, y, x].astype(f32) + peer[slot, g, y, x].astype(f32)

    def lead_stage(k):
        slot, st = lax.rem(k, IN_SLOTS), lax.rem(k, SEND_SLOTS)
        wait_bytes(own.at[slot], own_sem.at[slot])
        wait_bytes(peer.at[slot], peer_send.at[slot])
        wait_bytes(peer.at[slot], peer_recv.at[slot])

        @pl.when(k > SEND_SLOTS)
        def _():
            wait_bytes(lead.at[st], lead_send.at[st])

        @pl.when(k > 0)
        def _():
            for role, step in ((0, 2), (1, -1)):
                for g in range(GROUPS):
                    dest = at(first(g), step * SIGNS[g])
                    for o in range(RING):
                        lead[st, role, g, o] = pair(slot, g, dest, o)
                for g in range(GROUPS):
                    into, toward = ((r1, SIGNS[g]), (r2, -SIGNS[g]))[role]
                    remote(lead.at[st, role, g], into.at[k, g], lead_send.at[st], r_recv.at[role, k], near_first(g, toward)).start()

    def raw_leads():
        for role, step in ((0, 2), (1, -1)):
            for g in range(GROUPS):
                dest = at(first(g), step * SIGNS[g])
                toward = near_first(g, (SIGNS[g], -SIGNS[g])[role])
                for c in (core, 1 - core):
                    block = grads.at[g, :, dest, c] if X_FIRST[g] else grads.at[g, dest, :, c]
                    target = toward - core + c
                    remote(block, raw.at[role, g, core], raw_send, r_recv.at[role, 0], target).start()

    def raw_pair(role, g, o):
        return raw[role, g, 0, o].astype(f32) + raw[role, g, 1, o].astype(f32)

    def forward_stage(k):
        slot = lax.rem(k, IN_SLOTS)

        @pl.when(k == 0)
        def _():
            wait_bytes(raw.at[0], r_recv.at[0, 0])
            for g in range(GROUPS):
                dest = at(first(g), SIGNS[g])
                for o in range(RING):
                    r1[0, g, o] = raw_pair(0, g, o) + pair(0, g, dest, o)

        @pl.when(k > 0)
        def _():
            wait_bytes(r1.at[k], r_recv.at[0, k])
            for g in range(GROUPS):
                dest = at(first(g), SIGNS[g])
                for o in range(RING):
                    r1[k, g, o] = r1[k, g, o] + pair(slot, g, dest, o)

        for g in range(GROUPS):
            remote(r1.at[k, g], r3.at[k, g], fwd_send.at[k], r_recv.at[2, k], near_first(g, SIGNS[g])).start()

    def part_stage(k):
        slot = lax.rem(k, IN_SLOTS)
        wait_bytes(r3.at[k], r_recv.at[2, k])

        @pl.when(k == 0)
        def _():
            wait_bytes(raw.at[1], r_recv.at[1, 0])
            for g in range(GROUPS):
                for o in range(RING):
                    r3[0, g, o] = (r3[0, g, o] + raw_pair(1, g, o)) + pair(0, g, first(g), o)

        @pl.when(k > 0)
        def _():
            wait_bytes(r2.at[k], r_recv.at[1, k])
            for g in range(GROUPS):
                for o in range(RING):
                    r3[k, g, o] = (r3[k, g, o] + r2[k, g, o]) + pair(slot, g, first(g), o)


        @pl.when(k + IN_SLOTS < chunks)
        def _():
            pl.semaphore_signal(peer_free, inc=1, device_id={'data': buddy}, device_id_type=MESH)

        straight = k == chunks - 1
        for g in range(GROUPS):
            s = SIGNS[g]
            far = near_second(g, jnp.where(straight, 2 * s, s))
            remote(r3.at[k, g, at(second(g), 2 * s)], p1.at[k, g], part_send.at[k], p_recv.at[0, k], far).start()
            remote(r3.at[k, g, at(second(g), -s)], p2.at[k, g], part_send.at[k], p_recv.at[1, k], near_second(g, -s)).start()

            @pl.when(straight)
            def _():
                remote(r3.at[k, g, at(second(g), s)], p3.at[k, g], last_send.at[k], p_recv.at[2, k], near_second(g, s)).start()

    def last_stage(k):
        wait_bytes(p1.at[k], p_recv.at[0, k])

        @pl.when(k < chunks - 1)
        def _():
            for g in range(GROUPS):
                dest = at(second(g), SIGNS[g])
                p1[k, g] = p1[k, g] + r3[k, g, dest]
            for g in range(GROUPS):
                remote(p1.at[k, g], p3.at[k, g], last_send.at[k], p_recv.at[2, k], near_second(g, SIGNS[g])).start()

        @pl.when(k == chunks - 1)
        def _():
            for g in range(GROUPS):
                r3[k, g, second(g)] = r3[k, g, second(g)] + p1[k, g]

    def give(k):
        for g in range(GROUPS):
            j, slot, owner = k * m + g, k // per_slot, owner_of(k, g)

            @pl.when(owner != me)
            def _():
                remote(half_out.at[j], half_in.at[slot, me], half_send, half_recv.at[slot], owner).start()
                remote(sq_out.at[j], sq_in.at[slot, me], sq_send, sq_recv.at[slot], owner).start()

    def final_stage(k):
        @pl.when(k == 0)
        def _():
            wait_bytes(mom, mom_sem)

        wait_bytes(p2.at[k], p_recv.at[1, k])
        wait_bytes(p3.at[k], p_recv.at[2, k])
        for g in range(GROUPS):
            j = k * m + g
            total = r3[k, g, second(g)] + p2[k, g] + p3[k, g]
            new = MOMENTUM_COEF * mom[j] + total
            mom[j] = new
            short = new.astype(bf16)
            sq = jnp.sum(new * new, axis=0, keepdims=True)
            sq = functools.reduce(jnp.add, [sq[:, n * 128:(n + 1) * 128] for n in range(cols // 128)])
            half_out[j] = short
            sq_out[j] = sq

            @pl.when(owner_of(k, g) == me)
            def _():
                half_in[k // per_slot, me] = short
                sq_in[k // per_slot, me] = sq

        @pl.when(k < chunks - RING)
        def _():
            give(k)

        @pl.when(k == chunks - 1)
        def _():
            @pl.loop(chunks - RING, chunks)
            def _(late):
                give(late)

    def ns_start(slot):
        wait_bytes(half_in.at[slot, pl.ds(0, devs - 1)], half_recv.at[slot])
        wait_bytes(sq_in.at[slot, pl.ds(0, devs - 1)], sq_recv.at[slot])
        sq = jnp.sum(jnp.sum(sq_in[slot], axis=0), axis=1, keepdims=True)
        scale = jnp.sqrt(sq) + NORM_EPS

        @pl.loop(0, devs)
        def _(d):
            x_buf[slot, pl.ds(pl.multiple_of(d * rows, rows), rows), :] = (half_in[slot, d].astype(f32) / scale).astype(bf16)

    def ns_iter(slot):
        x = x_buf[slot]
        gram[...] = lax.dot_general(x, x, (((1,), (1,)), ((), ())), preferred_element_type=f32).astype(bf16)
        a = gram[...]
        poly[...] = (COEF_B * a.astype(f32) + COEF_C * jnp.dot(a, a, preferred_element_type=f32)).astype(bf16)
        x_buf[slot] = (COEF_A * x.astype(f32) + jnp.dot(poly[...], x, preferred_element_type=f32)).astype(bf16)

    def ns_iters(slot, lo, hi):
        @pl.loop(lo, hi)
        def _(_):
            ns_iter(slot)

    def x_block(slot, d):
        return x_buf.at[slot, pl.ds(pl.multiple_of(d * rows, rows), rows), :]

    def x_give(slot, part):
        j = mine(slot)
        recv = x_recv0 if slot == 0 else x_recv.at[slot - 1, my_turn]
        for dx in range(RING):
            for c in range(CORES):
                d = (lax.rem(py + dx + part, RING) * RING + lax.rem(px + dx, RING)) * CORES + c

                @pl.when(d != me)
                def _():
                    remote(x_block(slot, d), x_in.at[j], x_send.at[slot], recv, d).start()

    def x_give_all(slot):
        @pl.loop(0, RING)
        def _(part):
            x_give(slot, part)

    def x_keep(slot):
        x_in[mine(slot)] = x_buf[slot, pl.ds(pl.multiple_of(me * rows, rows), rows), :]

    def update(k):
        for g in range(GROUPS):
            j = k * m + g
            old = w[j]
            w[j] = old - LEARN_RATE * (x_in[j].astype(f32) * rms_scale + WEIGHT_DECAY * old)

    for k in range(AHEAD):
        fetch_own(jnp.int32(k))
    barrier = pltpu.get_barrier_semaphore()
    near = (buddy, device(at(px, 1), py), device(at(px, -1), py), device(px, at(py, 1)), device(px, at(py, -1)))
    near += tuple(d - core + 1 - core for d in near[1:])
    for d in near:
        pl.semaphore_signal(barrier, inc=1, device_id={'data': d}, device_id_type=MESH)
    pl.semaphore_wait(barrier, len(near))
    raw_leads()
    for k in range(AHEAD):
        fetch_peer(jnp.int32(k))
    pltpu.make_async_copy(mom_in, mom, mom_sem).start()
    pltpu.make_async_copy(w_in, w, w_sem).start()

    @pl.loop(0, chunks + 4)
    def _(t):
        @pl.when(t + AHEAD < chunks)
        def _():
            fetch_own(t + AHEAD)
            fetch_peer(t + AHEAD)

        for lag, stage in enumerate((lead_stage, forward_stage, part_stage, last_stage, final_stage)):
            @pl.when(jnp.logical_and(t >= lag, t < chunks + lag))
            def _():
                stage(t - lag)

        for slot in range(slots):
            begin = slot * per_slot + my_turn + 5

            @pl.when(jnp.logical_and(t == begin, begin <= chunks))
            def _():
                ns_start(slot)
                ns_iters(slot, 0, EARLY)

            @pl.when(jnp.logical_and(t == begin + 1, begin < chunks))
            def _():
                ns_iters(slot, EARLY, NS_ITERS)
                x_keep(slot)
    end = slots - 1
    busy = my_turn >= RING

    @pl.when(jnp.logical_not(busy))
    def _():
        x_give_all(0)

        @pl.when(my_turn == RING - 1)
        def _():
            ns_iters(end, EARLY, NS_ITERS)
            x_keep(end)

        x_give_all(end)

    @pl.when(busy)
    def _():
        ns_start(end)
        x_give_all(0)
        ns_iters(end, 0, NS_ITERS)
        x_keep(end)
        x_give_all(end)

    @pl.loop(0, chunks)
    def _(k):
        wait_bytes(r1.at[k], fwd_send.at[k])
        wait_bytes(p1.at[k], part_send.at[k])
        wait_bytes(p2.at[k], part_send.at[k])
        wait_bytes(p1.at[k], last_send.at[k])

    for st in range(SEND_SLOTS):
        wait_bytes(lead.at[st], lead_send.at[st])
    wait_bytes(raw, raw_send)
    wait_bytes(half_out.at[pl.ds(0, n_mats - slots)], half_send)
    wait_bytes(sq_out.at[pl.ds(0, n_mats - slots)], sq_send)
    wait_bytes(w, w_sem)
    wait_bytes(half_in.at[0, pl.ds(0, devs - 1)], x_recv0)

    @pl.loop(0, per_slot)
    def _(k):
        update(k)

    @pl.loop(0, per_slot)
    def _(turn):
        @pl.when(turn == my_turn)
        def _():
            wait_bytes(x_in.at[pl.ds(0, m - 1)], x_recv.at[0, turn])

        @pl.when(turn != my_turn)
        def _():
            wait_bytes(x_in.at[pl.ds(0, m)], x_recv.at[0, turn])

        update(per_slot + turn)

    for slot in range(slots):
        wait_bytes(half_in.at[slot, pl.ds(0, devs - 1)], x_send.at[slot])


def _store(mom, w, mom_out, w_out, sem):
    copies = [pltpu.make_async_copy(a, b, sem.at[n]) for n, (a, b) in enumerate(((mom, mom_out), (w, w_out)))]
    for copy in copies:
        copy.start()
    for copy in copies:
        copy.wait()


def store(mom, w):
    return pl.pallas_call(
        _store,
        out_shape=(jax.ShapeDtypeStruct(mom.shape, mom.dtype), jax.ShapeDtypeStruct(w.shape, w.dtype)),
        in_specs=[pl.BlockSpec(memory_space=pltpu.VMEM)] * 2,
        out_specs=(pl.BlockSpec(memory_space=pl.ANY),) * 2,
        scratch_shapes=[pltpu.SemaphoreType.DMA((2,))],
        compiler_params=pltpu.CompilerParams(vmem_limit_bytes=2**20),
    )(mom, w)


def muon(devs, grads, mom, w):
    n_mats, rows, cols = mom.shape
    n_rows = rows * devs
    m = GROUPS
    chunks = n_mats // m
    slots = n_mats // devs
    f32, bf16 = jnp.float32, jnp.bfloat16
    dma, vmem = pltpu.SemaphoreType.DMA, pltpu.VMEM
    grads = grads.reshape(n_mats, RING, RING, CORES, rows, cols)
    wide = (chunks, GROUPS, RING, rows, cols)
    thin = (chunks, GROUPS, rows, cols)
    return pl.pallas_call(
        functools.partial(_kernel, devs),
        out_shape=(
            vmem(mom.shape, f32),
            vmem(w.shape, f32),
        ),
        in_specs=[pl.BlockSpec(memory_space=pl.ANY)] * 3,
        out_specs=(pl.BlockSpec(memory_space=vmem),) * 2,
        scratch_shapes=[
            vmem((IN_SLOTS, m, RING, RING, rows, cols), bf16),
            vmem((IN_SLOTS, m, RING, RING, rows, cols), bf16),
            vmem(wide, f32), vmem(wide, f32), vmem(wide, f32),
            vmem(thin, f32), vmem(thin, f32), vmem(thin, f32),
            vmem((SEND_SLOTS, 2, GROUPS, RING, rows, cols), f32),
            vmem((2, GROUPS, CORES, RING, rows, cols), bf16),
            vmem(mom.shape, bf16),
            vmem((n_mats, 1, 128), f32),
            vmem((slots, devs, rows, cols), bf16),
            vmem((slots, devs, 1, 128), f32),
            vmem((slots, n_rows, cols), bf16),
            vmem(mom.shape, bf16),
            vmem((n_rows, n_rows), bf16),
            vmem((n_rows, n_rows), bf16),
            dma((IN_SLOTS,)), dma((IN_SLOTS,)), dma((IN_SLOTS,)), pltpu.SemaphoreType.REGULAR,
            dma((SEND_SLOTS,)), dma, dma((3, chunks)), dma((chunks,)), dma((3, chunks)), dma((chunks,)), dma((chunks,)),
            dma, dma, dma, dma, dma((slots,)), dma((slots,)), dma((slots,)), dma, dma((slots - 1, chunks // slots)),
        ],
        compiler_params=pltpu.CompilerParams(
            collective_id=0, has_side_effects=True, vmem_limit_bytes=57 * 2**20),
    )(grads, mom, w)


def solution(mesh):
    devs = mesh.shape['data']
    row_spec = P('stage', 'data', None)
    grad_spec = P(('stage', 'data'), None, None, None)

    def local_step(w_rows, mom_rows, grad_full):
        n_mats, rows_dev, n_cols = w_rows.shape
        assert devs == RING * RING * CORES and n_mats == 2 * devs and rows_dev * devs <= n_cols
        mom_new, w_new = store(*muon(devs, grad_full[0], mom_rows, w_rows))
        return w_new, mom_new

    return jax.shard_map(local_step, mesh=mesh, in_specs=(row_spec, row_spec, grad_spec), out_specs=(row_spec, row_spec), check_vma=False)
```

```python
import functools
import math

import jax
import jax.numpy as jnp
from jax import lax
from jax.experimental import pallas as pl
from jax.experimental.pallas import tpu as pltpu
from jax.sharding import PartitionSpec as P

MOMENTUM_COEF = 0.95
LEARN_RATE = 0.05
WEIGHT_DECAY = 0.2
NORM_EPS = 1e-7
COEF_A = 3.4445
COEF_B = -4.7750
COEF_C = 2.0315
NS_ITERS = 5
EARLY = 3

CORES = 2
RING = 4
SIGNS = (1, -1, 1, -1)
X_FIRST = (True, True, False, False)
GROUPS = 4
IN_SLOTS = 6
SEND_SLOTS = 3
AHEAD = 2
MESH = pl.DeviceIdType.MESH
TRIPS = sorted(
    ((x, y, c) for x in range(RING) for y in range(RING) for c in range(CORES) if x or y or c),
    key=lambda t: -min(t[0], RING - t[0]) - min(t[1], RING - t[1]))


def _kernel(
    devs, grads, mom_in, w_in, mom, w,
    own, peer, r1, r2, r3, p1, p2, p3, lead, raw, half_out, sq_out, half_in, sq_in, x_buf, x_in, gram, poly,
    own_sem, peer_send, peer_recv, peer_free, lead_send, raw_send, r_recv, fwd_send, p_recv, part_send, last_send,
    mom_sem, w_sem, half_send, sq_send, half_recv, sq_recv, x_send, x_recv0, x_recv,
):
    n_mats, rows, cols = mom.shape
    m = GROUPS
    chunks = n_mats // m
    slots = n_mats // devs
    per_slot = chunks // slots
    rms_scale = 0.2 * math.sqrt(max(rows * devs, cols))
    f32, bf16 = jnp.float32, jnp.bfloat16

    me = lax.axis_index('data')
    core = lax.rem(me, CORES)
    chip = me // CORES
    px, py = lax.rem(chip, RING), chip // RING
    buddy = me + 1 - 2 * core

    def at(pos, step):
        return lax.rem(pos + step + RING, RING)

    def device(x, y):
        return (y * RING + x) * CORES + core

    def first(g):
        return px if X_FIRST[g] else py

    def second(g):
        return py if X_FIRST[g] else px

    def near_first(g, step):
        return device(at(px, step), py) if X_FIRST[g] else device(px, at(py, step))

    def near_second(g, step):
        return device(px, at(py, step)) if X_FIRST[g] else device(at(px, step), py)

    def remote(src, dst, send, recv, target):
        return pltpu.make_async_remote_copy(
            src_ref=src, dst_ref=dst, send_sem=send, recv_sem=recv,
            device_id={'data': target}, device_id_type=MESH)

    def wait_bytes(ref, sem):
        pltpu.make_async_copy(ref, ref, sem).wait()

    def owner_of(k, g):
        kk = lax.rem(k, per_slot)
        return (g * RING + lax.rem(kk + g, RING)) * CORES + kk // RING

    my_turn = RING * core + at(px, -py)

    def mine(slot):
        return (slot * per_slot + my_turn) * m + py

    def fetch_own(k):
        slot = lax.rem(k, IN_SLOTS)
        pltpu.make_async_copy(grads.at[pl.ds(k * m, m), :, :, core], own.at[slot], own_sem.at[slot]).start()

    def fetch_peer(k):
        slot = lax.rem(k, IN_SLOTS)

        @pl.when(k >= IN_SLOTS)
        def _():
            pl.semaphore_wait(peer_free, 1)

        remote(grads.at[pl.ds(k * m, m), :, :, 1 - core], peer.at[slot], peer_send.at[slot], peer_recv.at[slot], buddy).start()

    def pair(slot, g, on_first, o):
        y, x = (o, on_first) if X_FIRST[g] else (on_first, o)
        return own[slot, g, y, x].astype(f32) + peer[slot, g, y, x].astype(f32)

    def lead_stage(k):
        slot, st = lax.rem(k, IN_SLOTS), lax.rem(k, SEND_SLOTS)
        wait_bytes(own.at[slot], own_sem.at[slot])
        wait_bytes(peer.at[slot], peer_send.at[slot])
        wait_bytes(peer.at[slot], peer_recv.at[slot])

        @pl.when(k > SEND_SLOTS)
        def _():
            wait_bytes(lead.at[st], lead_send.at[st])

        @pl.when(k > 0)
        def _():
            for role, step in ((0, 2), (1, -1)):
                for g in range(GROUPS):
                    dest = at(first(g), step * SIGNS[g])
                    for o in range(RING):
                        lead[st, role, g, o] = pair(slot, g, dest, o)
                for g in range(GROUPS):
                    into, toward = ((r1, SIGNS[g]), (r2, -SIGNS[g]))[role]
                    remote(lead.at[st, role, g], into.at[k, g], lead_send.at[st], r_recv.at[role, k], near_first(g, toward)).start()

    def raw_leads():
        for role, step in ((0, 2), (1, -1)):
            for g in range(GROUPS):
                dest = at(first(g), step * SIGNS[g])
                toward = near_first(g, (SIGNS[g], -SIGNS[g])[role])
                for c in (core, 1 - core):
                    block = grads.at[g, :, dest, c] if X_FIRST[g] else grads.at[g, dest, :, c]
                    target = toward - core + c
                    remote(block, raw.at[role, g, core], raw_send, r_recv.at[role, 0], target).start()

    def raw_pair(role, g, o):
        return raw[role, g, 0, o].astype(f32) + raw[role, g, 1, o].astype(f32)

    def forward_stage(k):
        slot = lax.rem(k, IN_SLOTS)

        @pl.when(k == 0)
        def _():
            wait_bytes(raw.at[0], r_recv.at[0, 0])
            for g in range(GROUPS):
                dest = at(first(g), SIGNS[g])
                for o in range(RING):
                    r1[0, g, o] = raw_pair(0, g, o) + pair(0, g, dest, o)

        @pl.when(k > 0)
        def _():
            wait_bytes(r1.at[k], r_recv.at[0, k])
            for g in range(GROUPS):
                dest = at(first(g), SIGNS[g])
                for o in range(RING):
                    r1[k, g, o] = r1[k, g, o] + pair(slot, g, dest, o)

        for g in range(GROUPS):
            remote(r1.at[k, g], r3.at[k, g], fwd_send.at[k], r_recv.at[2, k], near_first(g, SIGNS[g])).start()

    def part_stage(k):
        slot = lax.rem(k, IN_SLOTS)
        wait_bytes(r3.at[k], r_recv.at[2, k])

        @pl.when(k == 0)
        def _():
            wait_bytes(raw.at[1], r_recv.at[1, 0])
            for g in range(GROUPS):
                for o in range(RING):
                    r3[0, g, o] = (r3[0, g, o] + raw_pair(1, g, o)) + pair(0, g, first(g), o)

        @pl.when(k > 0)
        def _():
            wait_bytes(r2.at[k], r_recv.at[1, k])
            for g in range(GROUPS):
                for o in range(RING):
                    r3[k, g, o] = (r3[k, g, o] + r2[k, g, o]) + pair(slot, g, first(g), o)


        @pl.when(k + IN_SLOTS < chunks)
        def _():
            pl.semaphore_signal(peer_free, inc=1, device_id={'data': buddy}, device_id_type=MESH)

        straight = k == chunks - 1
        for g in range(GROUPS):
            s = SIGNS[g]
            far = near_second(g, jnp.where(straight, 2 * s, s))
            remote(r3.at[k, g, at(second(g), 2 * s)], p1.at[k, g], part_send.at[k], p_recv.at[0, k], far).start()
            remote(r3.at[k, g, at(second(g), -s)], p2.at[k, g], part_send.at[k], p_recv.at[1, k], near_second(g, -s)).start()

            @pl.when(straight)
            def _():
                remote(r3.at[k, g, at(second(g), s)], p3.at[k, g], last_send.at[k], p_recv.at[2, k], near_second(g, s)).start()

    def last_stage(k):
        wait_bytes(p1.at[k], p_recv.at[0, k])

        @pl.when(k < chunks - 1)
        def _():
            for g in range(GROUPS):
                dest = at(second(g), SIGNS[g])
                p1[k, g] = p1[k, g] + r3[k, g, dest]
            for g in range(GROUPS):
                remote(p1.at[k, g], p3.at[k, g], last_send.at[k], p_recv.at[2, k], near_second(g, SIGNS[g])).start()

        @pl.when(k == chunks - 1)
        def _():
            for g in range(GROUPS):
                r3[k, g, second(g)] = r3[k, g, second(g)] + p1[k, g]

    def give(k):
        for g in range(GROUPS):
            j, slot, owner = k * m + g, k // per_slot, owner_of(k, g)

            @pl.when(owner != me)
            def _():
                remote(half_out.at[j], half_in.at[slot, me], half_send, half_recv.at[slot], owner).start()
                remote(sq_out.at[j], sq_in.at[slot, me], sq_send, sq_recv.at[slot], owner).start()

    def final_stage(k):
        @pl.when(k == 0)
        def _():
            wait_bytes(mom, mom_sem)

        wait_bytes(p2.at[k], p_recv.at[1, k])
        wait_bytes(p3.at[k], p_recv.at[2, k])
        for g in range(GROUPS):
            j = k * m + g
            total = r3[k, g, second(g)] + p2[k, g] + p3[k, g]
            new = MOMENTUM_COEF * mom[j] + total
            mom[j] = new
            short = new.astype(bf16)
            sq = jnp.sum(new * new, axis=0, keepdims=True)
            sq = functools.reduce(jnp.add, [sq[:, n * 128:(n + 1) * 128] for n in range(cols // 128)])
            half_out[j] = short
            sq_out[j] = sq

            @pl.when(owner_of(k, g) == me)
            def _():
                half_in[k // per_slot, me] = short
                sq_in[k // per_slot, me] = sq

        @pl.when(k < per_slot)
        def _():
            give(k)

        @pl.when(k == chunks - 3)
        def _():
            @pl.loop(per_slot, chunks - RING)
            def _(late):
                give(late)

        @pl.when(k == chunks - 1)
        def _():
            @pl.loop(chunks - RING, chunks)
            def _(late):
                give(late)

    def ns_start(slot):
        wait_bytes(half_in.at[slot, pl.ds(0, devs - 1)], half_recv.at[slot])
        wait_bytes(sq_in.at[slot, pl.ds(0, devs - 1)], sq_recv.at[slot])
        sq = jnp.sum(jnp.sum(sq_in[slot], axis=0), axis=1, keepdims=True)
        scale = jnp.sqrt(sq) + NORM_EPS

        @pl.loop(0, devs)
        def _(d):
            x_buf[slot, pl.ds(pl.multiple_of(d * rows, rows), rows), :] = (half_in[slot, d].astype(f32) / scale).astype(bf16)

    def ns_iter(slot):
        x = x_buf[slot]
        gram[...] = lax.dot_general(x, x, (((1,), (1,)), ((), ())), preferred_element_type=f32).astype(bf16)
        a = gram[...]
        poly[...] = (COEF_B * a.astype(f32) + COEF_C * jnp.dot(a, a, preferred_element_type=f32)).astype(bf16)
        x_buf[slot] = (COEF_A * x.astype(f32) + jnp.dot(poly[...], x, preferred_element_type=f32)).astype(bf16)

    def ns_iters(slot, lo, hi):
        @pl.loop(lo, hi)
        def _(_):
            ns_iter(slot)

    def x_block(slot, d):
        return x_buf.at[slot, pl.ds(pl.multiple_of(d * rows, rows), rows), :]

    def x_give(slot, trips):
        j = mine(slot)
        recv = x_recv0 if slot == 0 else x_recv.at[slot - 1, my_turn]
        for dx, dy, other in trips:
            c = 1 - core if other else core
            d = (at(py, dy) * RING + at(px, dx)) * CORES + c
            remote(x_block(slot, d), x_in.at[j], x_send.at[slot], recv, d).start()

    def x_keep(slot):
        x_in[mine(slot)] = x_buf[slot, pl.ds(pl.multiple_of(me * rows, rows), rows), :]

    def update(k):
        for g in range(GROUPS):
            j = k * m + g
            old = w[j]
            w[j] = old - LEARN_RATE * (x_in[j].astype(f32) * rms_scale + WEIGHT_DECAY * old)

    for k in range(AHEAD):
        fetch_own(jnp.int32(k))
    barrier = pltpu.get_barrier_semaphore()
    near = (buddy, device(at(px, 1), py), device(at(px, -1), py), device(px, at(py, 1)), device(px, at(py, -1)))
    near += tuple(d - core + 1 - core for d in near[1:])
    for d in near:
        pl.semaphore_signal(barrier, inc=1, device_id={'data': d}, device_id_type=MESH)
    pl.semaphore_wait(barrier, len(near))
    raw_leads()
    for k in range(AHEAD):
        fetch_peer(jnp.int32(k))
    pltpu.make_async_copy(mom_in, mom, mom_sem).start()
    pltpu.make_async_copy(w_in, w, w_sem).start()

    @pl.loop(0, chunks + 4)
    def _(t):
        @pl.when(t + AHEAD < chunks)
        def _():
            fetch_own(t + AHEAD)
            fetch_peer(t + AHEAD)

        for lag, stage in enumerate((lead_stage, forward_stage, part_stage, last_stage, final_stage)):
            @pl.when(jnp.logical_and(t >= lag, t < chunks + lag))
            def _():
                stage(t - lag)

        begin = my_turn + 5

        @pl.when(t == begin)
        def _():
            ns_start(0)
            ns_iters(0, 0, EARLY)

        @pl.when(t == begin + 1)
        def _():
            ns_iters(0, EARLY, NS_ITERS)
            x_keep(0)

    end = slots - 1
    ns_start(end)
    for i in range(NS_ITERS):
        x_give(0, TRIPS[i::NS_ITERS])
        ns_iter(end)
    x_keep(end)
    x_give(end, TRIPS)

    @pl.loop(0, chunks)
    def _(k):
        wait_bytes(r1.at[k], fwd_send.at[k])
        wait_bytes(p1.at[k], part_send.at[k])
        wait_bytes(p2.at[k], part_send.at[k])
        wait_bytes(p1.at[k], last_send.at[k])

    for st in range(SEND_SLOTS):
        wait_bytes(lead.at[st], lead_send.at[st])
    wait_bytes(raw, raw_send)
    wait_bytes(half_out.at[pl.ds(0, n_mats - slots)], half_send)
    wait_bytes(sq_out.at[pl.ds(0, n_mats - slots)], sq_send)
    wait_bytes(w, w_sem)
    wait_bytes(half_in.at[0, pl.ds(0, devs - 1)], x_recv0)

    @pl.loop(0, per_slot)
    def _(k):
        update(k)

    @pl.loop(0, per_slot)
    def _(turn):
        @pl.when(turn == my_turn)
        def _():
            wait_bytes(x_in.at[pl.ds(0, m - 1)], x_recv.at[0, turn])

        @pl.when(turn != my_turn)
        def _():
            wait_bytes(x_in.at[pl.ds(0, m)], x_recv.at[0, turn])

        update(per_slot + turn)

    for slot in range(slots):
        wait_bytes(half_in.at[slot, pl.ds(0, devs - 1)], x_send.at[slot])


def _store(mom, w, mom_out, w_out, sem):
    copies = [pltpu.make_async_copy(a, b, sem.at[n]) for n, (a, b) in enumerate(((mom, mom_out), (w, w_out)))]
    for copy in copies:
        copy.start()
    for copy in copies:
        copy.wait()


def store(mom, w):
    return pl.pallas_call(
        _store,
        out_shape=(jax.ShapeDtypeStruct(mom.shape, mom.dtype), jax.ShapeDtypeStruct(w.shape, w.dtype)),
        in_specs=[pl.BlockSpec(memory_space=pltpu.VMEM)] * 2,
        out_specs=(pl.BlockSpec(memory_space=pl.ANY),) * 2,
        scratch_shapes=[pltpu.SemaphoreType.DMA((2,))],
        compiler_params=pltpu.CompilerParams(vmem_limit_bytes=2**20),
    )(mom, w)


def muon(devs, grads, mom, w):
    n_mats, rows, cols = mom.shape
    n_rows = rows * devs
    m = GROUPS
    chunks = n_mats // m
    slots = n_mats // devs
    f32, bf16 = jnp.float32, jnp.bfloat16
    dma, vmem = pltpu.SemaphoreType.DMA, pltpu.VMEM
    grads = grads.reshape(n_mats, RING, RING, CORES, rows, cols)
    wide = (chunks, GROUPS, RING, rows, cols)
    thin = (chunks, GROUPS, rows, cols)
    return pl.pallas_call(
        functools.partial(_kernel, devs),
        out_shape=(
            vmem(mom.shape, f32),
            vmem(w.shape, f32),
        ),
        in_specs=[pl.BlockSpec(memory_space=pl.ANY)] * 3,
        out_specs=(pl.BlockSpec(memory_space=vmem),) * 2,
        scratch_shapes=[
            vmem((IN_SLOTS, m, RING, RING, rows, cols), bf16),
            vmem((IN_SLOTS, m, RING, RING, rows, cols), bf16),
            vmem(wide, f32), vmem(wide, f32), vmem(wide, f32),
            vmem(thin, f32), vmem(thin, f32), vmem(thin, f32),
            vmem((SEND_SLOTS, 2, GROUPS, RING, rows, cols), f32),
            vmem((2, GROUPS, CORES, RING, rows, cols), bf16),
            vmem(mom.shape, bf16),
            vmem((n_mats, 1, 128), f32),
            vmem((slots, devs, rows, cols), bf16),
            vmem((slots, devs, 1, 128), f32),
            vmem((slots, n_rows, cols), bf16),
            vmem(mom.shape, bf16),
            vmem((n_rows, n_rows), bf16),
            vmem((n_rows, n_rows), bf16),
            dma((IN_SLOTS,)), dma((IN_SLOTS,)), dma((IN_SLOTS,)), pltpu.SemaphoreType.REGULAR,
            dma((SEND_SLOTS,)), dma, dma((3, chunks)), dma((chunks,)), dma((3, chunks)), dma((chunks,)), dma((chunks,)),
            dma, dma, dma, dma, dma((slots,)), dma((slots,)), dma((slots,)), dma, dma((slots - 1, chunks // slots)),
        ],
        compiler_params=pltpu.CompilerParams(
            collective_id=0, has_side_effects=True, vmem_limit_bytes=57 * 2**20),
    )(grads, mom, w)


def solution(mesh):
    devs = mesh.shape['data']
    row_spec = P('stage', 'data', None)
    grad_spec = P(('stage', 'data'), None, None, None)

    def local_step(w_rows, mom_rows, grad_full):
        n_mats, rows_dev, n_cols = w_rows.shape
        assert devs == RING * RING * CORES and n_mats == 2 * devs and rows_dev * devs <= n_cols
        mom_new, w_new = store(*muon(devs, grad_full[0], mom_rows, w_rows))
        return w_new, mom_new

    return jax.shard_map(local_step, mesh=mesh, in_specs=(row_spec, row_spec, grad_spec), out_specs=(row_spec, row_spec), check_vma=False)
```

```python
import functools
import math

import jax
import jax.numpy as jnp
from jax import lax
from jax.experimental import pallas as pl
from jax.experimental.pallas import tpu as pltpu
from jax.sharding import PartitionSpec as P

MOMENTUM_COEF = 0.95
LEARN_RATE = 0.05
WEIGHT_DECAY = 0.2
NORM_EPS = 1e-7
COEF_A = 3.4445
COEF_B = -4.7750
COEF_C = 2.0315
NS_ITERS = 5
EARLY = 3

CORES = 2
RING = 4
SIGNS = (1, -1, 1, -1)
X_FIRST = (True, True, False, False)
GROUPS = 4
IN_SLOTS = 6
SEND_SLOTS = 3
AHEAD = 2
MESH = pl.DeviceIdType.MESH
WAYS = sorted(
    ((x, y) for x in range(RING) for y in range(RING)),
    key=lambda t: -min(t[0], RING - t[0]) - min(t[1], RING - t[1]))
TRIPS = [(x, y, c) for x, y in WAYS for c in range(CORES) if x or y or c]


def _kernel(
    devs, grads, mom_in, w_in, mom, w,
    own, peer, r1, r2, r3, p1, p2, p3, lead, raw, half_out, sq_out, half_in, sq_in, x_buf, x_in, gram, poly,
    own_sem, peer_send, peer_recv, peer_free, lead_send, raw_send, r_recv, fwd_send, p_recv, part_send, last_send,
    mom_sem, w_sem, half_send, sq_send, half_recv, sq_recv, x_send, x_recv0, x_recv,
):
    n_mats, rows, cols = mom.shape
    m = GROUPS
    chunks = n_mats // m
    slots = n_mats // devs
    per_slot = chunks // slots
    rms_scale = 0.2 * math.sqrt(max(rows * devs, cols))
    f32, bf16 = jnp.float32, jnp.bfloat16

    me = lax.axis_index('data')
    core = lax.rem(me, CORES)
    chip = me // CORES
    px, py = lax.rem(chip, RING), chip // RING
    buddy = me + 1 - 2 * core

    def at(pos, step):
        return lax.rem(pos + step + RING, RING)

    def device(x, y):
        return (y * RING + x) * CORES + core

    def first(g):
        return px if X_FIRST[g] else py

    def second(g):
        return py if X_FIRST[g] else px

    def near_first(g, step):
        return device(at(px, step), py) if X_FIRST[g] else device(px, at(py, step))

    def near_second(g, step):
        return device(px, at(py, step)) if X_FIRST[g] else device(at(px, step), py)

    def remote(src, dst, send, recv, target):
        return pltpu.make_async_remote_copy(
            src_ref=src, dst_ref=dst, send_sem=send, recv_sem=recv,
            device_id={'data': target}, device_id_type=MESH)

    def wait_bytes(ref, sem):
        pltpu.make_async_copy(ref, ref, sem).wait()

    def owner_of(k, g):
        kk = lax.rem(k, per_slot)
        return (g * RING + lax.rem(kk + g, RING)) * CORES + kk // RING

    my_turn = RING * core + at(px, -py)

    def mine(slot):
        return (slot * per_slot + my_turn) * m + py

    def fetch_own(k):
        slot = lax.rem(k, IN_SLOTS)
        pltpu.make_async_copy(grads.at[pl.ds(k * m, m), :, :, core], own.at[slot], own_sem.at[slot]).start()

    def fetch_peer(k):
        slot = lax.rem(k, IN_SLOTS)

        @pl.when(k >= IN_SLOTS)
        def _():
            pl.semaphore_wait(peer_free, 1)

        remote(grads.at[pl.ds(k * m, m), :, :, 1 - core], peer.at[slot], peer_send.at[slot], peer_recv.at[slot], buddy).start()

    def pair(slot, g, on_first, o):
        y, x = (o, on_first) if X_FIRST[g] else (on_first, o)
        return own[slot, g, y, x].astype(f32) + peer[slot, g, y, x].astype(f32)

    def lead_stage(k):
        slot, st = lax.rem(k, IN_SLOTS), lax.rem(k, SEND_SLOTS)
        wait_bytes(own.at[slot], own_sem.at[slot])
        wait_bytes(peer.at[slot], peer_send.at[slot])
        wait_bytes(peer.at[slot], peer_recv.at[slot])

        @pl.when(k > SEND_SLOTS)
        def _():
            wait_bytes(lead.at[st], lead_send.at[st])

        @pl.when(k > 0)
        def _():
            for role, step in ((0, 2), (1, -1)):
                for g in range(GROUPS):
                    dest = at(first(g), step * SIGNS[g])
                    for o in range(RING):
                        lead[st, role, g, o] = pair(slot, g, dest, o)
                for g in range(GROUPS):
                    into, toward = ((r1, SIGNS[g]), (r2, -SIGNS[g]))[role]
                    remote(lead.at[st, role, g], into.at[k, g], lead_send.at[st], r_recv.at[role, k], near_first(g, toward)).start()

    def raw_leads():
        for role, step in ((0, 2), (1, -1)):
            for g in range(GROUPS):
                dest = at(first(g), step * SIGNS[g])
                toward = near_first(g, (SIGNS[g], -SIGNS[g])[role])
                for c in (core, 1 - core):
                    block = grads.at[g, :, dest, c] if X_FIRST[g] else grads.at[g, dest, :, c]
                    target = toward - core + c
                    remote(block, raw.at[role, g, core], raw_send, r_recv.at[role, 0], target).start()

    def raw_pair(role, g, o):
        return raw[role, g, 0, o].astype(f32) + raw[role, g, 1, o].astype(f32)

    def forward_stage(k):
        slot = lax.rem(k, IN_SLOTS)

        @pl.when(k == 0)
        def _():
            wait_bytes(raw.at[0], r_recv.at[0, 0])
            for g in range(GROUPS):
                dest = at(first(g), SIGNS[g])
                for o in range(RING):
                    r1[0, g, o] = raw_pair(0, g, o) + pair(0, g, dest, o)

        @pl.when(k > 0)
        def _():
            wait_bytes(r1.at[k], r_recv.at[0, k])
            for g in range(GROUPS):
                dest = at(first(g), SIGNS[g])
                for o in range(RING):
                    r1[k, g, o] = r1[k, g, o] + pair(slot, g, dest, o)

        for g in range(GROUPS):
            remote(r1.at[k, g], r3.at[k, g], fwd_send.at[k], r_recv.at[2, k], near_first(g, SIGNS[g])).start()

    def part_stage(k):
        slot = lax.rem(k, IN_SLOTS)
        wait_bytes(r3.at[k], r_recv.at[2, k])

        @pl.when(k == 0)
        def _():
            wait_bytes(raw.at[1], r_recv.at[1, 0])
            for g in range(GROUPS):
                for o in range(RING):
                    r3[0, g, o] = (r3[0, g, o] + raw_pair(1, g, o)) + pair(0, g, first(g), o)

        @pl.when(k > 0)
        def _():
            wait_bytes(r2.at[k], r_recv.at[1, k])
            for g in range(GROUPS):
                for o in range(RING):
                    r3[k, g, o] = (r3[k, g, o] + r2[k, g, o]) + pair(slot, g, first(g), o)


        @pl.when(k + IN_SLOTS < chunks)
        def _():
            pl.semaphore_signal(peer_free, inc=1, device_id={'data': buddy}, device_id_type=MESH)

        straight = k == chunks - 1
        for g in range(GROUPS):
            s = SIGNS[g]
            far = near_second(g, jnp.where(straight, 2 * s, s))
            remote(r3.at[k, g, at(second(g), 2 * s)], p1.at[k, g], part_send.at[k], p_recv.at[0, k], far).start()
            remote(r3.at[k, g, at(second(g), -s)], p2.at[k, g], part_send.at[k], p_recv.at[1, k], near_second(g, -s)).start()

            @pl.when(straight)
            def _():
                remote(r3.at[k, g, at(second(g), s)], p3.at[k, g], last_send.at[k], p_recv.at[2, k], near_second(g, s)).start()

    def last_stage(k):
        wait_bytes(p1.at[k], p_recv.at[0, k])

        @pl.when(k < chunks - 1)
        def _():
            for g in range(GROUPS):
                dest = at(second(g), SIGNS[g])
                p1[k, g] = p1[k, g] + r3[k, g, dest]
            for g in range(GROUPS):
                remote(p1.at[k, g], p3.at[k, g], last_send.at[k], p_recv.at[2, k], near_second(g, SIGNS[g])).start()

        @pl.when(k == chunks - 1)
        def _():
            for g in range(GROUPS):
                r3[k, g, second(g)] = r3[k, g, second(g)] + p1[k, g]

    def give(k):
        for g in range(GROUPS):
            j, slot, owner = k * m + g, k // per_slot, owner_of(k, g)

            @pl.when(owner != me)
            def _():
                remote(half_out.at[j], half_in.at[slot, me], half_send, half_recv.at[slot], owner).start()
                remote(sq_out.at[j], sq_in.at[slot, me], sq_send, sq_recv.at[slot], owner).start()

    def give_block(slot, c):
        for dx, dy in WAYS:
            tx, ty = at(px, dx), at(py, dy)
            j, owner = (slot * per_slot + RING * c + at(tx, -ty)) * m + ty, (ty * RING + tx) * CORES + c

            def send():
                remote(half_out.at[j], half_in.at[slot, me], half_send, half_recv.at[slot], owner).start()
                remote(sq_out.at[j], sq_in.at[slot, me], sq_send, sq_recv.at[slot], owner).start()

            if dx or dy:
                send()
            else:
                pl.when(core != c)(send)

    def final_stage(k):
        @pl.when(k == 0)
        def _():
            wait_bytes(mom, mom_sem)

        wait_bytes(p2.at[k], p_recv.at[1, k])
        wait_bytes(p3.at[k], p_recv.at[2, k])
        for g in range(GROUPS):
            j = k * m + g
            total = r3[k, g, second(g)] + p2[k, g] + p3[k, g]
            new = MOMENTUM_COEF * mom[j] + total
            mom[j] = new
            short = new.astype(bf16)
            sq = jnp.sum(new * new, axis=0, keepdims=True)
            sq = functools.reduce(jnp.add, [sq[:, n * 128:(n + 1) * 128] for n in range(cols // 128)])
            half_out[j] = short
            sq_out[j] = sq

            @pl.when(owner_of(k, g) == me)
            def _():
                half_in[k // per_slot, me] = short
                sq_in[k // per_slot, me] = sq

        @pl.when(k < per_slot)
        def _():
            give(k)

        @pl.when(k == chunks - 3)
        def _():
            give_block(slots - 1, 0)

        @pl.when(k == chunks - 1)
        def _():
            give_block(slots - 1, 1)

    def ns_start(slot):
        wait_bytes(half_in.at[slot, pl.ds(0, devs - 1)], half_recv.at[slot])
        wait_bytes(sq_in.at[slot, pl.ds(0, devs - 1)], sq_recv.at[slot])
        sq = jnp.sum(jnp.sum(sq_in[slot], axis=0), axis=1, keepdims=True)
        scale = jnp.sqrt(sq) + NORM_EPS

        @pl.loop(0, devs)
        def _(d):
            x_buf[slot, pl.ds(pl.multiple_of(d * rows, rows), rows), :] = (half_in[slot, d].astype(f32) / scale).astype(bf16)

    def ns_iter(slot):
        x = x_buf[slot]
        gram[...] = lax.dot_general(x, x, (((1,), (1,)), ((), ())), preferred_element_type=f32).astype(bf16)
        a = gram[...]
        poly[...] = (COEF_B * a.astype(f32) + COEF_C * jnp.dot(a, a, preferred_element_type=f32)).astype(bf16)
        x_buf[slot] = (COEF_A * x.astype(f32) + jnp.dot(poly[...], x, preferred_element_type=f32)).astype(bf16)

    def ns_iters(slot, lo, hi):
        @pl.loop(lo, hi)
        def _(_):
            ns_iter(slot)

    def x_block(slot, d):
        return x_buf.at[slot, pl.ds(pl.multiple_of(d * rows, rows), rows), :]

    def x_give(slot, trips):
        j = mine(slot)
        recv = x_recv0 if slot == 0 else x_recv.at[slot - 1, my_turn]
        for dx, dy, other in trips:
            c = 1 - core if other else core
            d = (at(py, dy) * RING + at(px, dx)) * CORES + c
            remote(x_block(slot, d), x_in.at[j], x_send.at[slot], recv, d).start()

    def x_keep(slot):
        x_in[mine(slot)] = x_buf[slot, pl.ds(pl.multiple_of(me * rows, rows), rows), :]

    def update(k):
        for g in range(GROUPS):
            j = k * m + g
            old = w[j]
            w[j] = old - LEARN_RATE * (x_in[j].astype(f32) * rms_scale + WEIGHT_DECAY * old)

    for k in range(AHEAD):
        fetch_own(jnp.int32(k))
    barrier = pltpu.get_barrier_semaphore()
    near = (buddy, device(at(px, 1), py), device(at(px, -1), py), device(px, at(py, 1)), device(px, at(py, -1)))
    near += tuple(d - core + 1 - core for d in near[1:])
    for d in near:
        pl.semaphore_signal(barrier, inc=1, device_id={'data': d}, device_id_type=MESH)
    pl.semaphore_wait(barrier, len(near))
    raw_leads()
    for k in range(AHEAD):
        fetch_peer(jnp.int32(k))
    pltpu.make_async_copy(mom_in, mom, mom_sem).start()
    pltpu.make_async_copy(w_in, w, w_sem).start()

    @pl.loop(0, chunks + 4)
    def _(t):
        @pl.when(t + AHEAD < chunks)
        def _():
            fetch_own(t + AHEAD)
            fetch_peer(t + AHEAD)

        for lag, stage in enumerate((lead_stage, forward_stage, part_stage, last_stage, final_stage)):
            @pl.when(jnp.logical_and(t >= lag, t < chunks + lag))
            def _():
                stage(t - lag)

        begin = my_turn + 5

        @pl.when(t == begin)
        def _():
            ns_start(0)
            ns_iters(0, 0, EARLY)

        @pl.when(t == begin + 1)
        def _():
            ns_iters(0, EARLY, NS_ITERS)
            x_keep(0)

    end = slots - 1
    ns_start(end)
    for i in range(NS_ITERS):
        x_give(0, TRIPS[i::NS_ITERS])
        ns_iter(end)
    x_keep(end)
    x_give(end, TRIPS)

    @pl.loop(0, chunks)
    def _(k):
        wait_bytes(r1.at[k], fwd_send.at[k])
        wait_bytes(p1.at[k], part_send.at[k])
        wait_bytes(p2.at[k], part_send.at[k])
        wait_bytes(p1.at[k], last_send.at[k])

    for st in range(SEND_SLOTS):
        wait_bytes(lead.at[st], lead_send.at[st])
    wait_bytes(raw, raw_send)
    wait_bytes(half_out.at[pl.ds(0, n_mats - slots)], half_send)
    wait_bytes(sq_out.at[pl.ds(0, n_mats - slots)], sq_send)
    wait_bytes(w, w_sem)
    wait_bytes(half_in.at[0, pl.ds(0, devs - 1)], x_recv0)

    @pl.loop(0, per_slot)
    def _(k):
        update(k)

    @pl.loop(0, per_slot)
    def _(turn):
        @pl.when(turn == my_turn)
        def _():
            wait_bytes(x_in.at[pl.ds(0, m - 1)], x_recv.at[0, turn])

        @pl.when(turn != my_turn)
        def _():
            wait_bytes(x_in.at[pl.ds(0, m)], x_recv.at[0, turn])

        update(per_slot + turn)

    for slot in range(slots):
        wait_bytes(half_in.at[slot, pl.ds(0, devs - 1)], x_send.at[slot])


def _store(mom, w, mom_out, w_out, sem):
    copies = [pltpu.make_async_copy(a, b, sem.at[n]) for n, (a, b) in enumerate(((mom, mom_out), (w, w_out)))]
    for copy in copies:
        copy.start()
    for copy in copies:
        copy.wait()


def store(mom, w):
    return pl.pallas_call(
        _store,
        out_shape=(jax.ShapeDtypeStruct(mom.shape, mom.dtype), jax.ShapeDtypeStruct(w.shape, w.dtype)),
        in_specs=[pl.BlockSpec(memory_space=pltpu.VMEM)] * 2,
        out_specs=(pl.BlockSpec(memory_space=pl.ANY),) * 2,
        scratch_shapes=[pltpu.SemaphoreType.DMA((2,))],
        compiler_params=pltpu.CompilerParams(vmem_limit_bytes=2**20),
    )(mom, w)


def muon(devs, grads, mom, w):
    n_mats, rows, cols = mom.shape
    n_rows = rows * devs
    m = GROUPS
    chunks = n_mats // m
    slots = n_mats // devs
    f32, bf16 = jnp.float32, jnp.bfloat16
    dma, vmem = pltpu.SemaphoreType.DMA, pltpu.VMEM
    grads = grads.reshape(n_mats, RING, RING, CORES, rows, cols)
    wide = (chunks, GROUPS, RING, rows, cols)
    thin = (chunks, GROUPS, rows, cols)
    return pl.pallas_call(
        functools.partial(_kernel, devs),
        out_shape=(
            vmem(mom.shape, f32),
            vmem(w.shape, f32),
        ),
        in_specs=[pl.BlockSpec(memory_space=pl.ANY)] * 3,
        out_specs=(pl.BlockSpec(memory_space=vmem),) * 2,
        scratch_shapes=[
            vmem((IN_SLOTS, m, RING, RING, rows, cols), bf16),
            vmem((IN_SLOTS, m, RING, RING, rows, cols), bf16),
            vmem(wide, f32), vmem(wide, f32), vmem(wide, f32),
            vmem(thin, f32), vmem(thin, f32), vmem(thin, f32),
            vmem((SEND_SLOTS, 2, GROUPS, RING, rows, cols), f32),
            vmem((2, GROUPS, CORES, RING, rows, cols), bf16),
            vmem(mom.shape, bf16),
            vmem((n_mats, 1, 128), f32),
            vmem((slots, devs, rows, cols), bf16),
            vmem((slots, devs, 1, 128), f32),
            vmem((slots, n_rows, cols), bf16),
            vmem(mom.shape, bf16),
            vmem((n_rows, n_rows), bf16),
            vmem((n_rows, n_rows), bf16),
            dma((IN_SLOTS,)), dma((IN_SLOTS,)), dma((IN_SLOTS,)), pltpu.SemaphoreType.REGULAR,
            dma((SEND_SLOTS,)), dma, dma((3, chunks)), dma((chunks,)), dma((3, chunks)), dma((chunks,)), dma((chunks,)),
            dma, dma, dma, dma, dma((slots,)), dma((slots,)), dma((slots,)), dma, dma((slots - 1, chunks // slots)),
        ],
        compiler_params=pltpu.CompilerParams(
            collective_id=0, has_side_effects=True, vmem_limit_bytes=57 * 2**20),
    )(grads, mom, w)


def solution(mesh):
    devs = mesh.shape['data']
    row_spec = P('stage', 'data', None)
    grad_spec = P(('stage', 'data'), None, None, None)

    def local_step(w_rows, mom_rows, grad_full):
        n_mats, rows_dev, n_cols = w_rows.shape
        assert devs == RING * RING * CORES and n_mats == 2 * devs and rows_dev * devs <= n_cols
        mom_new, w_new = store(*muon(devs, grad_full[0], mom_rows, w_rows))
        return w_new, mom_new

    return jax.shard_map(local_step, mesh=mesh, in_specs=(row_spec, row_spec, grad_spec), out_specs=(row_spec, row_spec), check_vma=False)
```

```python
import functools
import math

import jax
import jax.numpy as jnp
from jax import lax
from jax.experimental import pallas as pl
from jax.experimental.pallas import tpu as pltpu
from jax.sharding import PartitionSpec as P

MOMENTUM_COEF = 0.95
LEARN_RATE = 0.05
WEIGHT_DECAY = 0.2
NORM_EPS = 1e-7
COEF_A = 3.4445
COEF_B = -4.7750
COEF_C = 2.0315
NS_ITERS = 5
EARLY = 3

CORES = 2
RING = 4
SIGNS = (1, -1, 1, -1)
X_FIRST = (True, True, False, False)
GROUPS = 4
IN_SLOTS = 6
SEND_SLOTS = 3
AHEAD = 2
MESH = pl.DeviceIdType.MESH
WAYS = sorted(
    ((x, y) for x in range(RING) for y in range(RING)),
    key=lambda t: -min(t[0], RING - t[0]) - min(t[1], RING - t[1]))
TRIPS = [(x, y, c) for x, y in WAYS for c in range(CORES) if x or y or c]


def _kernel(
    devs, grads, mom_in, w_in, mom, w,
    own, peer, r1, r2, r3, p1, p2, p3, lead, raw, half_out, sq_out, half_in, sq_in, x_buf, x_in, gram, poly,
    own_sem, peer_send, peer_recv, peer_free, lead_send, raw_send, r_recv, fwd_send, p_recv, part_send, last_send,
    mom_sem, w_sem, half_send, sq_send, half_recv, sq_recv, x_send, x_recv0, x_recv,
):
    n_mats, rows, cols = mom.shape
    m = GROUPS
    chunks = n_mats // m
    slots = n_mats // devs
    per_slot = chunks // slots
    rms_scale = 0.2 * math.sqrt(max(rows * devs, cols))
    f32, bf16 = jnp.float32, jnp.bfloat16

    me = lax.axis_index('data')
    core = lax.rem(me, CORES)
    chip = me // CORES
    px, py = lax.rem(chip, RING), chip // RING
    buddy = me + 1 - 2 * core

    def at(pos, step):
        return lax.rem(pos + step + RING, RING)

    def device(x, y):
        return (y * RING + x) * CORES + core

    def first(g):
        return px if X_FIRST[g] else py

    def second(g):
        return py if X_FIRST[g] else px

    def near_first(g, step):
        return device(at(px, step), py) if X_FIRST[g] else device(px, at(py, step))

    def near_second(g, step):
        return device(px, at(py, step)) if X_FIRST[g] else device(at(px, step), py)

    def remote(src, dst, send, recv, target):
        return pltpu.make_async_remote_copy(
            src_ref=src, dst_ref=dst, send_sem=send, recv_sem=recv,
            device_id={'data': target}, device_id_type=MESH)

    def wait_bytes(ref, sem):
        pltpu.make_async_copy(ref, ref, sem).wait()

    def owner_of(k, g):
        kk = lax.rem(k, per_slot)
        return (g * RING + lax.rem(kk + g, RING)) * CORES + kk // RING

    my_turn = RING * core + at(px, -py)

    def mine(slot):
        return (slot * per_slot + my_turn) * m + py

    def fetch_own(k):
        slot = lax.rem(k, IN_SLOTS)
        pltpu.make_async_copy(grads.at[pl.ds(k * m, m), :, :, core], own.at[slot], own_sem.at[slot]).start()

    def fetch_peer(k):
        slot = lax.rem(k, IN_SLOTS)

        @pl.when(k >= IN_SLOTS)
        def _():
            pl.semaphore_wait(peer_free, 1)

        remote(grads.at[pl.ds(k * m, m), :, :, 1 - core], peer.at[slot], peer_send.at[slot], peer_recv.at[slot], buddy).start()

    def pair(slot, g, on_first, o):
        y, x = (o, on_first) if X_FIRST[g] else (on_first, o)
        return own[slot, g, y, x].astype(f32) + peer[slot, g, y, x].astype(f32)

    def lead_stage(k):
        slot, st = lax.rem(k, IN_SLOTS), lax.rem(k, SEND_SLOTS)
        wait_bytes(own.at[slot], own_sem.at[slot])
        wait_bytes(peer.at[slot], peer_send.at[slot])
        wait_bytes(peer.at[slot], peer_recv.at[slot])

        @pl.when(k > SEND_SLOTS)
        def _():
            wait_bytes(lead.at[st], lead_send.at[st])

        @pl.when(k > 0)
        def _():
            for role, step in ((0, 2), (1, -1)):
                for g in range(GROUPS):
                    dest = at(first(g), step * SIGNS[g])
                    for o in range(RING):
                        lead[st, role, g, o] = pair(slot, g, dest, o)
                for g in range(GROUPS):
                    into, toward = ((r1, SIGNS[g]), (r2, -SIGNS[g]))[role]
                    remote(lead.at[st, role, g], into.at[k, g], lead_send.at[st], r_recv.at[role, k], near_first(g, toward)).start()

    def raw_leads():
        for role, step in ((0, 2), (1, -1)):
            for g in range(GROUPS):
                dest = at(first(g), step * SIGNS[g])
                toward = near_first(g, (SIGNS[g], -SIGNS[g])[role])
                for c in (core, 1 - core):
                    block = grads.at[g, :, dest, c] if X_FIRST[g] else grads.at[g, dest, :, c]
                    target = toward - core + c
                    remote(block, raw.at[role, g, core], raw_send, r_recv.at[role, 0], target).start()

    def raw_pair(role, g, o):
        return raw[role, g, 0, o].astype(f32) + raw[role, g, 1, o].astype(f32)

    def forward_stage(k):
        slot = lax.rem(k, IN_SLOTS)

        @pl.when(k == 0)
        def _():
            wait_bytes(raw.at[0], r_recv.at[0, 0])
            for g in range(GROUPS):
                dest = at(first(g), SIGNS[g])
                for o in range(RING):
                    r1[0, g, o] = raw_pair(0, g, o) + pair(0, g, dest, o)

        @pl.when(k > 0)
        def _():
            wait_bytes(r1.at[k], r_recv.at[0, k])
            for g in range(GROUPS):
                dest = at(first(g), SIGNS[g])
                for o in range(RING):
                    r1[k, g, o] = r1[k, g, o] + pair(slot, g, dest, o)

        for g in range(GROUPS):
            remote(r1.at[k, g], r3.at[k, g], fwd_send.at[k], r_recv.at[2, k], near_first(g, SIGNS[g])).start()

    def part_stage(k):
        slot = lax.rem(k, IN_SLOTS)
        wait_bytes(r3.at[k], r_recv.at[2, k])

        @pl.when(k == 0)
        def _():
            wait_bytes(raw.at[1], r_recv.at[1, 0])
            for g in range(GROUPS):
                for o in range(RING):
                    r3[0, g, o] = (r3[0, g, o] + raw_pair(1, g, o)) + pair(0, g, first(g), o)

        @pl.when(k > 0)
        def _():
            wait_bytes(r2.at[k], r_recv.at[1, k])
            for g in range(GROUPS):
                for o in range(RING):
                    r3[k, g, o] = (r3[k, g, o] + r2[k, g, o]) + pair(slot, g, first(g), o)


        @pl.when(k + IN_SLOTS < chunks)
        def _():
            pl.semaphore_signal(peer_free, inc=1, device_id={'data': buddy}, device_id_type=MESH)

        straight = k == chunks - 1
        for g in range(GROUPS):
            s = SIGNS[g]
            far = near_second(g, jnp.where(straight, 2 * s, s))
            remote(r3.at[k, g, at(second(g), 2 * s)], p1.at[k, g], part_send.at[k], p_recv.at[0, k], far).start()
            remote(r3.at[k, g, at(second(g), -s)], p2.at[k, g], part_send.at[k], p_recv.at[1, k], near_second(g, -s)).start()

            @pl.when(straight)
            def _():
                remote(r3.at[k, g, at(second(g), s)], p3.at[k, g], last_send.at[k], p_recv.at[2, k], near_second(g, s)).start()

        @pl.when(straight)
        def _():
            give_block(slots - 1, 0)

    def last_stage(k):
        wait_bytes(p1.at[k], p_recv.at[0, k])

        @pl.when(k < chunks - 1)
        def _():
            for g in range(GROUPS):
                dest = at(second(g), SIGNS[g])
                p1[k, g] = p1[k, g] + r3[k, g, dest]
            for g in range(GROUPS):
                remote(p1.at[k, g], p3.at[k, g], last_send.at[k], p_recv.at[2, k], near_second(g, SIGNS[g])).start()

        @pl.when(k == chunks - 1)
        def _():
            for g in range(GROUPS):
                r3[k, g, second(g)] = r3[k, g, second(g)] + p1[k, g]

    def give(k):
        for g in range(GROUPS):
            j, slot, owner = k * m + g, k // per_slot, owner_of(k, g)

            @pl.when(owner != me)
            def _():
                remote(half_out.at[j], half_in.at[slot, me], half_send, half_recv.at[slot], owner).start()
                remote(sq_out.at[j], sq_in.at[slot, me], sq_send, sq_recv.at[slot], owner).start()

    def give_block(slot, c):
        for dx, dy in WAYS:
            tx, ty = at(px, dx), at(py, dy)
            j, owner = (slot * per_slot + RING * c + at(tx, -ty)) * m + ty, (ty * RING + tx) * CORES + c

            def send():
                remote(half_out.at[j], half_in.at[slot, me], half_send, half_recv.at[slot], owner).start()
                remote(sq_out.at[j], sq_in.at[slot, me], sq_send, sq_recv.at[slot], owner).start()

            if dx or dy:
                send()
            else:
                pl.when(core != c)(send)

    def final_stage(k):
        @pl.when(k == 0)
        def _():
            wait_bytes(mom, mom_sem)

        wait_bytes(p2.at[k], p_recv.at[1, k])
        wait_bytes(p3.at[k], p_recv.at[2, k])
        for g in range(GROUPS):
            j = k * m + g
            total = r3[k, g, second(g)] + p2[k, g] + p3[k, g]
            new = MOMENTUM_COEF * mom[j] + total
            mom[j] = new
            short = new.astype(bf16)
            sq = jnp.sum(new * new, axis=0, keepdims=True)
            sq = functools.reduce(jnp.add, [sq[:, n * 128:(n + 1) * 128] for n in range(cols // 128)])
            half_out[j] = short
            sq_out[j] = sq

            @pl.when(owner_of(k, g) == me)
            def _():
                half_in[k // per_slot, me] = short
                sq_in[k // per_slot, me] = sq

        @pl.when(k < per_slot)
        def _():
            give(k)

        @pl.when(k == chunks - 1)
        def _():
            give_block(slots - 1, 1)

    def ns_start(slot):
        wait_bytes(half_in.at[slot, pl.ds(0, devs - 1)], half_recv.at[slot])
        wait_bytes(sq_in.at[slot, pl.ds(0, devs - 1)], sq_recv.at[slot])
        sq = jnp.sum(jnp.sum(sq_in[slot], axis=0), axis=1, keepdims=True)
        scale = jnp.sqrt(sq) + NORM_EPS

        @pl.loop(0, devs)
        def _(d):
            x_buf[slot, pl.ds(pl.multiple_of(d * rows, rows), rows), :] = (half_in[slot, d].astype(f32) / scale).astype(bf16)

    def ns_iter(slot):
        x = x_buf[slot]
        gram[...] = lax.dot_general(x, x, (((1,), (1,)), ((), ())), preferred_element_type=f32).astype(bf16)
        a = gram[...]
        poly[...] = (COEF_B * a.astype(f32) + COEF_C * jnp.dot(a, a, preferred_element_type=f32)).astype(bf16)
        x_buf[slot] = (COEF_A * x.astype(f32) + jnp.dot(poly[...], x, preferred_element_type=f32)).astype(bf16)

    def ns_iters(slot, lo, hi):
        @pl.loop(lo, hi)
        def _(_):
            ns_iter(slot)

    def x_block(slot, d):
        return x_buf.at[slot, pl.ds(pl.multiple_of(d * rows, rows), rows), :]

    def x_give(slot, trips):
        j = mine(slot)
        recv = x_recv0 if slot == 0 else x_recv.at[slot - 1, my_turn]
        for dx, dy, other in trips:
            c = 1 - core if other else core
            d = (at(py, dy) * RING + at(px, dx)) * CORES + c
            remote(x_block(slot, d), x_in.at[j], x_send.at[slot], recv, d).start()

    def x_keep(slot):
        x_in[mine(slot)] = x_buf[slot, pl.ds(pl.multiple_of(me * rows, rows), rows), :]

    def update(k):
        for g in range(GROUPS):
            j = k * m + g
            old = w[j]
            w[j] = old - LEARN_RATE * (x_in[j].astype(f32) * rms_scale + WEIGHT_DECAY * old)

    for k in range(AHEAD):
        fetch_own(jnp.int32(k))
    barrier = pltpu.get_barrier_semaphore()
    near = (buddy, device(at(px, 1), py), device(at(px, -1), py), device(px, at(py, 1)), device(px, at(py, -1)))
    near += tuple(d - core + 1 - core for d in near[1:])
    for d in near:
        pl.semaphore_signal(barrier, inc=1, device_id={'data': d}, device_id_type=MESH)
    pl.semaphore_wait(barrier, len(near))
    raw_leads()
    for k in range(AHEAD):
        fetch_peer(jnp.int32(k))
    pltpu.make_async_copy(mom_in, mom, mom_sem).start()
    pltpu.make_async_copy(w_in, w, w_sem).start()

    @pl.loop(0, chunks + 4)
    def _(t):
        @pl.when(t + AHEAD < chunks)
        def _():
            fetch_own(t + AHEAD)
            fetch_peer(t + AHEAD)

        for lag, stage in enumerate((lead_stage, forward_stage, part_stage, last_stage, final_stage)):
            @pl.when(jnp.logical_and(t >= lag, t < chunks + lag))
            def _():
                stage(t - lag)

        begin = my_turn + 5

        @pl.when(t == begin)
        def _():
            ns_start(0)
            ns_iters(0, 0, EARLY)

        @pl.when(t == begin + 1)
        def _():
            ns_iters(0, EARLY, NS_ITERS)
            x_keep(0)

    end = slots - 1
    ns_start(end)
    for i in range(NS_ITERS):
        x_give(0, TRIPS[i::NS_ITERS])
        ns_iter(end)
    x_keep(end)
    x_give(end, TRIPS)

    @pl.loop(0, chunks)
    def _(k):
        wait_bytes(r1.at[k], fwd_send.at[k])
        wait_bytes(p1.at[k], part_send.at[k])
        wait_bytes(p2.at[k], part_send.at[k])
        wait_bytes(p1.at[k], last_send.at[k])

    for st in range(SEND_SLOTS):
        wait_bytes(lead.at[st], lead_send.at[st])
    wait_bytes(raw, raw_send)
    wait_bytes(half_out.at[pl.ds(0, n_mats - slots)], half_send)
    wait_bytes(sq_out.at[pl.ds(0, n_mats - slots)], sq_send)
    wait_bytes(w, w_sem)
    wait_bytes(half_in.at[0, pl.ds(0, devs - 1)], x_recv0)

    @pl.loop(0, per_slot)
    def _(k):
        update(k)

    @pl.loop(0, per_slot)
    def _(turn):
        @pl.when(turn == my_turn)
        def _():
            wait_bytes(x_in.at[pl.ds(0, m - 1)], x_recv.at[0, turn])

        @pl.when(turn != my_turn)
        def _():
            wait_bytes(x_in.at[pl.ds(0, m)], x_recv.at[0, turn])

        update(per_slot + turn)

    for slot in range(slots):
        wait_bytes(half_in.at[slot, pl.ds(0, devs - 1)], x_send.at[slot])


def _store(mom, w, mom_out, w_out, sem):
    copies = [pltpu.make_async_copy(a, b, sem.at[n]) for n, (a, b) in enumerate(((mom, mom_out), (w, w_out)))]
    for copy in copies:
        copy.start()
    for copy in copies:
        copy.wait()


def store(mom, w):
    return pl.pallas_call(
        _store,
        out_shape=(jax.ShapeDtypeStruct(mom.shape, mom.dtype), jax.ShapeDtypeStruct(w.shape, w.dtype)),
        in_specs=[pl.BlockSpec(memory_space=pltpu.VMEM)] * 2,
        out_specs=(pl.BlockSpec(memory_space=pl.ANY),) * 2,
        scratch_shapes=[pltpu.SemaphoreType.DMA((2,))],
        compiler_params=pltpu.CompilerParams(vmem_limit_bytes=2**20),
    )(mom, w)


def muon(devs, grads, mom, w):
    n_mats, rows, cols = mom.shape
    n_rows = rows * devs
    m = GROUPS
    chunks = n_mats // m
    slots = n_mats // devs
    f32, bf16 = jnp.float32, jnp.bfloat16
    dma, vmem = pltpu.SemaphoreType.DMA, pltpu.VMEM
    grads = grads.reshape(n_mats, RING, RING, CORES, rows, cols)
    wide = (chunks, GROUPS, RING, rows, cols)
    thin = (chunks, GROUPS, rows, cols)
    return pl.pallas_call(
        functools.partial(_kernel, devs),
        out_shape=(
            vmem(mom.shape, f32),
            vmem(w.shape, f32),
        ),
        in_specs=[pl.BlockSpec(memory_space=pl.ANY)] * 3,
        out_specs=(pl.BlockSpec(memory_space=vmem),) * 2,
        scratch_shapes=[
            vmem((IN_SLOTS, m, RING, RING, rows, cols), bf16),
            vmem((IN_SLOTS, m, RING, RING, rows, cols), bf16),
            vmem(wide, f32), vmem(wide, f32), vmem(wide, f32),
            vmem(thin, f32), vmem(thin, f32), vmem(thin, f32),
            vmem((SEND_SLOTS, 2, GROUPS, RING, rows, cols), f32),
            vmem((2, GROUPS, CORES, RING, rows, cols), bf16),
            vmem(mom.shape, bf16),
            vmem((n_mats, 1, 128), f32),
            vmem((slots, devs, rows, cols), bf16),
            vmem((slots, devs, 1, 128), f32),
            vmem((slots, n_rows, cols), bf16),
            vmem(mom.shape, bf16),
            vmem((n_rows, n_rows), bf16),
            vmem((n_rows, n_rows), bf16),
            dma((IN_SLOTS,)), dma((IN_SLOTS,)), dma((IN_SLOTS,)), pltpu.SemaphoreType.REGULAR,
            dma((SEND_SLOTS,)), dma, dma((3, chunks)), dma((chunks,)), dma((3, chunks)), dma((chunks,)), dma((chunks,)),
            dma, dma, dma, dma, dma((slots,)), dma((slots,)), dma((slots,)), dma, dma((slots - 1, chunks // slots)),
        ],
        compiler_params=pltpu.CompilerParams(
            collective_id=0, has_side_effects=True, vmem_limit_bytes=57 * 2**20),
    )(grads, mom, w)


def solution(mesh):
    devs = mesh.shape['data']
    row_spec = P('stage', 'data', None)
    grad_spec = P(('stage', 'data'), None, None, None)

    def local_step(w_rows, mom_rows, grad_full):
        n_mats, rows_dev, n_cols = w_rows.shape
        assert devs == RING * RING * CORES and n_mats == 2 * devs and rows_dev * devs <= n_cols
        mom_new, w_new = store(*muon(devs, grad_full[0], mom_rows, w_rows))
        return w_new, mom_new

    return jax.shard_map(local_step, mesh=mesh, in_specs=(row_spec, row_spec, grad_spec), out_specs=(row_spec, row_spec), check_vma=False)
```
